8 devices in a mesh: tp: 4 (over z, y, x), cp: 2 (over core).
Axes of the slice: x: 2, y: 2, z: 1, core: 2. Of those that a mesh axis runs over, the one named last changes fastest.
Arguments:
- hidden: bfloat16 [8, 1024, 6144], P(None, 'cp')
- grad_out: bfloat16 [8, 1024, 6144], P(None, 'cp')
- w_query: bfloat16 [6144, 48, 128], P(None, 'tp')
- w_key: bfloat16 [6144, 128], replicated
- w_value: bfloat16 [6144, 128], replicated
- w_out: bfloat16 [48, 128, 6144], P('tp')
Outputs:
- output 1: bfloat16 [8, 1024, 6144], P(None, 'cp')
- output 2: bfloat16 [8, 1024, 6144], P(None, 'cp')
- output 3: float32 [6144, 48, 128], P(None, 'tp')
- output 4: float32 [6144, 128], replicated
- output 5: float32 [6144, 128], replicated
- output 6: float32 [48, 128, 6144], P('tp')
All inputs are finite; a program needn't handle non-finite values.
Results may differ from the reference program's by a relative error of at most 0.0110935.
Values are sent between devices in bfloat16 or wider.
A program may use at most 1.25 GiB of HBM per device.

```python
import jax
import jax.numpy as jnp
from jax import lax

BATCH = 8
SEQ = 1024
D_MODEL = 6144
HEADS = 48
HEAD_DIM = 128
Q_ROWS = 128


def rope_tables(positions):
    half_dim = HEAD_DIM // 2
    inv_freq = 1.0 / jnp.power(10000.0, jnp.arange(half_dim, dtype=jnp.float32) * (2.0 / HEAD_DIM))
    angles = positions.astype(jnp.float32)[:, None] * inv_freq[None, :]
    return jnp.cos(angles), jnp.sin(angles)


def rotate(rot_in, cos_tab, sin_tab):
    half_dim = rot_in.shape[-1] // 2
    low_half = rot_in[..., :half_dim]
    high_half = rot_in[..., half_dim:]
    return jnp.concatenate([low_half * cos_tab - high_half * sin_tab, high_half * cos_tab + low_half * sin_tab], axis=-1)


def unrotate(rot_in, cos_tab, sin_tab):
    half_dim = rot_in.shape[-1] // 2
    low_half = rot_in[..., :half_dim]
    high_half = rot_in[..., half_dim:]
    return jnp.concatenate([low_half * cos_tab + high_half * sin_tab, high_half * cos_tab - low_half * sin_tab], axis=-1)


def setup_inputs(seed: int = 0) -> dict:
    sub_keys = jax.random.split(jax.random.key(seed), 6)
    hidden = jax.random.normal(sub_keys[0], (BATCH, SEQ, D_MODEL), jnp.float32)
    grad_out = jax.random.normal(sub_keys[1], (BATCH, SEQ, D_MODEL), jnp.float32)
    in_scale = D_MODEL ** -0.5
    w_query = jax.random.normal(sub_keys[2], (D_MODEL, HEADS, HEAD_DIM), jnp.float32) * in_scale
    w_key = jax.random.normal(sub_keys[3], (D_MODEL, HEAD_DIM), jnp.float32) * in_scale
    w_value = jax.random.normal(sub_keys[4], (D_MODEL, HEAD_DIM), jnp.float32) * in_scale
    w_out = jax.random.normal(sub_keys[5], (HEADS, HEAD_DIM, D_MODEL), jnp.float32) * (HEADS * HEAD_DIM) ** -0.5
    return {"hidden": hidden.astype(jnp.bfloat16), "grad_out": grad_out.astype(jnp.bfloat16), "w_query": w_query.astype(jnp.bfloat16), "w_key": w_key.astype(jnp.bfloat16), "w_value": w_value.astype(jnp.bfloat16), "w_out": w_out.astype(jnp.bfloat16)}


def reference(hidden, grad_out, w_query, w_key, w_value, w_out):
    q_scale = HEAD_DIM ** -0.5
    n_blocks = SEQ // Q_ROWS
    cos_tab, sin_tab = rope_tables(jnp.arange(SEQ))
    flat_hidden = hidden.reshape(BATCH * SEQ, D_MODEL)
    key_pre = jnp.dot(flat_hidden, w_key, preferred_element_type=jnp.float32).reshape(BATCH, SEQ, HEAD_DIM)
    key_rot = rotate(key_pre, cos_tab, sin_tab).astype(jnp.bfloat16).astype(jnp.float32)
    val_all = jnp.dot(flat_hidden, w_value, preferred_element_type=jnp.float32).reshape(BATCH, SEQ, HEAD_DIM).astype(jnp.bfloat16).astype(jnp.float32)
    key_pos = jnp.arange(SEQ)
    hid_blocks = hidden.reshape(BATCH, n_blocks, Q_ROWS, D_MODEL).transpose(1, 0, 2, 3)
    grad_blocks = grad_out.reshape(BATCH, n_blocks, Q_ROWS, D_MODEL).transpose(1, 0, 2, 3)
    cos_blocks = cos_tab.reshape(n_blocks, Q_ROWS, HEAD_DIM // 2)
    sin_blocks = sin_tab.reshape(n_blocks, Q_ROWS, HEAD_DIM // 2)
    row_starts = jnp.arange(n_blocks) * Q_ROWS
    kv_zero = jnp.zeros((BATCH, SEQ, HEAD_DIM), jnp.float32)
    big_zero = jnp.zeros((BATCH, SEQ, D_MODEL), jnp.float32)

    def head_step(carry_in, head_weights):
        out_acc, dh_acc, dk_acc, dv_acc = carry_in
        wq_head, wo_head = head_weights

        def block_step(block_carry, block_in):
            dk_run, dv_run, dwq_run, dwo_run = block_carry
            hid_blk, grad_blk, cos_blk, sin_blk, row_start = block_in
            hid_flat = hid_blk.reshape(BATCH * Q_ROWS, D_MODEL)
            grad_flat = grad_blk.reshape(BATCH * Q_ROWS, D_MODEL)
            q_pre = jnp.dot(hid_flat, wq_head, preferred_element_type=jnp.float32).reshape(BATCH, Q_ROWS, HEAD_DIM)
            q_rot = (rotate(q_pre, cos_blk, sin_blk) * q_scale).astype(jnp.bfloat16).astype(jnp.float32)
            scores = jnp.einsum("bqe,bke->bqk", q_rot, key_rot)
            q_pos = row_start + jnp.arange(Q_ROWS)
            allowed = key_pos[None, :] <= q_pos[:, None]
            scores = jnp.where(allowed[None], scores, -jnp.inf)
            probs_blk = jax.nn.softmax(scores, axis=-1)
            attn_blk = jnp.einsum("bqk,bke->bqe", probs_blk, val_all).astype(jnp.bfloat16)
            d_attn = jnp.dot(grad_flat, wo_head.T, preferred_element_type=jnp.float32).astype(jnp.bfloat16)
            attn_f = attn_blk.astype(jnp.float32)
            d_attn_f = d_attn.astype(jnp.float32).reshape(BATCH, Q_ROWS, HEAD_DIM)
            d_prob = jnp.einsum("bqe,bke->bqk", d_attn_f, val_all)
            row_delta = jnp.sum(d_attn_f * attn_f, axis=-1, keepdims=True)
            d_score = probs_blk * (d_prob - row_delta)
            dq_blk = jnp.einsum("bqk,bke->bqe", d_score, key_rot)
            dk_run = dk_run + jnp.einsum("bqk,bqe->bke", d_score, q_rot)
            dv_run = dv_run + jnp.einsum("bqk,bqe->bke", probs_blk, d_attn_f)
            dq_pre = (unrotate(dq_blk, cos_blk, sin_blk) * q_scale).astype(jnp.bfloat16).reshape(BATCH * Q_ROWS, HEAD_DIM)
            attn_flat = attn_blk.reshape(BATCH * Q_ROWS, HEAD_DIM)
            dwq_run = dwq_run + jnp.dot(hid_flat.T, dq_pre, preferred_element_type=jnp.float32)
            dwo_run = dwo_run + jnp.dot(attn_flat.T, grad_flat, preferred_element_type=jnp.float32)
            out_part = jnp.dot(attn_flat, wo_head, preferred_element_type=jnp.float32)
            dh_part = jnp.dot(dq_pre, wq_head.T, preferred_element_type=jnp.float32)
            return (dk_run, dv_run, dwq_run, dwo_run), (out_part, dh_part)

        block_init = (kv_zero, kv_zero, jnp.zeros((D_MODEL, HEAD_DIM), jnp.float32), jnp.zeros((HEAD_DIM, D_MODEL), jnp.float32))
        block_out, block_ys = lax.scan(block_step, block_init, (hid_blocks, grad_blocks, cos_blocks, sin_blocks, row_starts))
        dk_run, dv_run, dwq_run, dwo_run = block_out
        out_parts, dh_parts = block_ys
        out_head = out_parts.reshape(n_blocks, BATCH, Q_ROWS, D_MODEL).transpose(1, 0, 2, 3).reshape(BATCH, SEQ, D_MODEL)
        dh_head = dh_parts.reshape(n_blocks, BATCH, Q_ROWS, D_MODEL).transpose(1, 0, 2, 3).reshape(BATCH, SEQ, D_MODEL)
        new_carry = (out_acc + out_head, dh_acc + dh_head, dk_acc + dk_run, dv_acc + dv_run)
        return new_carry, (dwq_run, dwo_run)

    head_init = (big_zero, big_zero, kv_zero, kv_zero)
    head_out, head_ys = lax.scan(head_step, head_init, (w_query.transpose(1, 0, 2), w_out))
    out_acc, dh_acc, dk_acc, dv_acc = head_out
    d_w_query = head_ys[0].transpose(1, 0, 2)
    d_w_out = head_ys[1]
    dk_pre = unrotate(dk_acc, cos_tab, sin_tab).astype(jnp.bfloat16).reshape(BATCH * SEQ, HEAD_DIM)
    dv_pre = dv_acc.astype(jnp.bfloat16).reshape(BATCH * SEQ, HEAD_DIM)
    d_w_key = jnp.dot(flat_hidden.T, dk_pre, preferred_element_type=jnp.float32)
    d_w_value = jnp.dot(flat_hidden.T, dv_pre, preferred_element_type=jnp.float32)
    dh_kv = jnp.dot(dk_pre, w_key.T, preferred_element_type=jnp.float32) + jnp.dot(dv_pre, w_value.T, preferred_element_type=jnp.float32)
    d_hidden = (dh_acc + dh_kv.reshape(BATCH, SEQ, D_MODEL)).astype(jnp.bfloat16)
    attn_out = out_acc.astype(jnp.bfloat16)
    return attn_out, d_hidden, d_w_query, d_w_key, d_w_value, d_w_out
```

```python
import functools

import jax
import jax.numpy as jnp
from jax import lax
from jax.experimental import pallas as pl
from jax.experimental.pallas import tpu as pltpu
from jax.sharding import PartitionSpec as P


F32 = jnp.float32
BF16 = jnp.bfloat16
ROPE_BASE = 10000.0
VMEM_LIMIT = 67043328
PIECE = 512
SUB = 256
E = 128
HALF = E // 2
ROWS = 2 * PIECE
N_SUB = ROWS // SUB
N_TILE = N_SUB * (N_SUB + 1) // 2
GROUP = 6
UNIT = 3
WIDE = GROUP * E
COLS = 512
DW_COLS = 1024
SCALE = E**-0.5


def rope_angles(n_pos):
    inv_freq = 1.0 / jnp.power(ROPE_BASE, jnp.arange(HALF, dtype=F32) * (2.0 / E))
    angles = jnp.arange(n_pos).astype(F32)[:, None] * inv_freq[None, :]
    return jnp.cos(angles), jnp.sin(angles)


def dot_nn(a, b):
    return jnp.dot(a, b, preferred_element_type=F32)


def dot_nt(a, b):
    return lax.dot_general(a, b, (((1,), (1,)), ((), ())), preferred_element_type=F32)


def lanes(parts):
    return jnp.concatenate(parts, axis=1)


def stack(parts):
    return jnp.concatenate(parts, axis=0)


def rows(p):
    return slice(PIECE * p, PIECE * (p + 1))


def heads(e):
    return slice(E * e, E * (e + 1))


def spec(block, index=None):
    rank = len(block)

    def full(*a):
        i = tuple(index(*a)) if index else ()
        return i + (0,) * (rank - len(i))

    mode = {} if index else {"pipeline_mode": pl.Buffered(1)}
    return pl.BlockSpec(block, full, **mode)


def struct(dtype, *shape):
    return jax.ShapeDtypeStruct(shape, dtype)


def call(body, grid, scal, ins, in_specs, outs, out_specs, flops, scratch=(), aliases=None):
    nbytes = sum(x.size * x.dtype.itemsize for x in jax.tree.leaves([ins, outs]))
    return pl.pallas_call(
        body,
        grid_spec=pltpu.PrefetchScalarGridSpec(
            num_scalar_prefetch=1, grid=grid, in_specs=in_specs, out_specs=out_specs, scratch_shapes=scratch
        ),
        out_shape=outs,
        input_output_aliases=aliases or {},
        cost_estimate=pl.CostEstimate(flops=int(flops), bytes_accessed=int(nbytes), transcendentals=0),
        compiler_params=pltpu.CompilerParams(vmem_limit_bytes=VMEM_LIMIT),
    )(scal, *ins)


def seq_of(l, s):
    return 2 * jnp.where(l == 0, s[0], 3 - s[0]) + s[1]


CHUNKS = 4


def proj_body(kind, n_w, n_kv, steps, nl, l0, s_ref, x_ref, r_ref, *refs):
    queries = kind == "q"
    if queries:
        cos_ref, sin_ref, *refs = refs
    w_refs, kv_refs, refs = refs[:n_w], refs[n_w : n_w + n_kv], refs[n_w + n_kv :]
    *outs, a_buf, w_buf, kv_buf, a_sem, w_sem, kv_sem = refs
    l, n = pl.program_id(0), pl.program_id(1)
    first = jnp.logical_and(l == 0, n == 0)
    d = x_ref.shape[-1]
    depth = d // CHUNKS
    c = s_ref[1]
    whole = slice(None)
    per = n_w // steps if n_w > 1 else 1

    def cut(k):
        return whole if k is None else pl.ds(k * depth, depth)

    def row_copies(i, k=None):
        return [
            pltpu.make_async_copy(src.at[at, :, cut(k)], a_buf.at[i, p, :, cut(k)], a_sem.at[i, p, k or 0])
            for p, (src, at) in enumerate(((x_ref, seq_of(i + l0, s_ref)), (r_ref, i + l0)))
        ]

    def weight_copies(j, k=None):
        copies = []
        for m in range(per):
            size = GROUP // per
            to = pl.ds(GROUP * j + size * m, size)
            src = w_refs[per * j + m] if n_w > 1 else w_refs[0]
            at = whole if n_w > 1 else pl.ds(GROUP * jnp.bitwise_xor(j, c), GROUP)
            at, to = ((at, cut(k)), (to, cut(k))) if queries else ((at, whole, cut(k)), (to, whole, cut(k)))
            copies.append(pltpu.make_async_copy(src.at[at], w_buf.at[to], w_sem.at[j, m, k or 0]))
        return copies

    def kv_copies():
        return [pltpu.make_async_copy(r, kv_buf.at[i], kv_sem.at[i]) for i, r in enumerate(kv_refs)]

    def wait(copies):
        for copy in copies:
            copy.wait()

    def product(i, h, k):
        a = stack([a_buf[i, p, :, cut(k)] for p in range(2)])
        if queries:
            return dot_nn(a, lanes([w_buf[h + e, cut(k), :] for e in range(GROUP)]))
        w = w_buf[pl.ds(h, GROUP), :, cut(k)]
        return dot_nt(a, w.reshape(WIDE, w.shape[2]))

    starts = [pl.multiple_of(PIECE * jnp.bitwise_xor(p, c), PIECE) for p in range(2)]

    def rotated(x, p):
        at = pl.ds(starts[p], PIECE)
        return x * cos_ref[at, :] + pltpu.roll(x, HALF, 1) * sin_ref[at, :]

    def store(x):
        for p in range(2):
            for e in range(GROUP):
                part = x[rows(p), heads(e)]
                outs[-1][p, e] = (rotated(part, p) * SCALE if queries else part).astype(BF16)

    @pl.when(first)
    def _():
        for k in range(CHUNKS):
            for copy in row_copies(0, k) + weight_copies(0, k):
                copy.start()
        later = [weight_copies(j) for j in range(1, steps)] + [kv_copies()] + [row_copies(i) for i in range(1, nl)]
        for copy in sum(later, []):
            copy.start()
        for k in range(CHUNKS):
            wait(row_copies(0, k) + weight_copies(0, k))
            part = product(0, 0, k)
            acc = part if k == 0 else acc + part
        store(acc)

    for i in range(1, nl):

        @pl.when(jnp.logical_and(l == i, n == 0))
        def _():
            wait(row_copies(i))

    for j in range(1, steps):

        @pl.when(jnp.logical_and(l == 0, n == j))
        def _():
            wait(weight_copies(j))

    @pl.when(jnp.logical_and(jnp.logical_not(first), n < steps))
    def _():
        store(product(l, GROUP * n, None))

    if n_kv:

        @pl.when(n == steps)
        def _():
            @pl.when(l == 0)
            def _():
                wait(kv_copies())

            x = dot_nn(stack([a_buf[l, p] for p in range(2)]), lanes([kv_buf[i] for i in range(n_kv)]))
            for p in range(2):
                outs[0][p] = rotated(x[rows(p), :E], p).astype(BF16)
                outs[1][p] = x[rows(p), E:].astype(BF16)


def proj(scal, kind, x, x_recv, weights, tables=(), kv=(), l0=0, nl=2):
    d = x.shape[-1]
    steps = 2 if len(weights) == 1 else len(weights) // 2
    hbm = pl.BlockSpec(memory_space=pl.ANY)
    kv_out = [struct(BF16, nl, 2, PIECE, E)] * len(kv)
    shape = (d, E) if kind == "q" else (E, d)
    dma = lambda *n: pltpu.SemaphoreType.DMA(n)
    return call(
        functools.partial(proj_body, kind, len(weights), len(kv), steps, nl, l0),
        (nl, steps + len(kv) // 2),
        scal,
        [x, x_recv, *tables, *weights, *kv],
        [hbm] * 2 + [spec((ROWS, E))] * len(tables) + [hbm] * (len(weights) + len(kv)),
        kv_out + [struct(BF16, nl, 2, steps * GROUP, PIECE, E)],
        [spec((None, 2, PIECE, E), lambda l, n, s: (l,))] * len(kv)
        + [spec((None, 2, GROUP, PIECE, E), lambda l, n, s: (l, 0, jnp.minimum(n, steps - 1)))],
        2 * nl * ROWS * d * steps * WIDE,
        scratch=[
            pltpu.VMEM((nl, 2, PIECE, d), BF16),
            pltpu.VMEM((steps * GROUP, *shape), BF16),
            pltpu.VMEM((len(kv) or 1, d if kv else GROUP, E), BF16),
            dma(nl, 2, CHUNKS),
            dma(steps, 2, CHUNKS),
            dma(2),
        ],
    )


def attn_body(mode, turned, s_ref, *refs):
    it = iter(refs)
    fwd, bwd = mode != "bwd", mode != "fwd"
    q_ref, k_ref, v_ref = next(it), next(it), next(it)
    if bwd:
        do_ref, cos_ref, sin_ref = next(it), next(it), next(it)
    if not fwd:
        ot_ref, lse_ref = next(it), next(it)
    if fwd:
        o_ref = next(it)
    if not bwd:
        ot_ref, lse_ref = next(it), next(it)
    if bwd:
        dq_ref, dk_ref, dv_ref = next(it), next(it), next(it)
    if turned:
        t_ref = next(it)
    keys, vals, keys_t, vals_t, s_buf, p_buf, ds_buf = it
    slot = [jnp.bitwise_xor(p, s_ref[1]) for p in range(2)]

    @pl.when(pl.program_id(1) == 0)
    def _():
        for p in range(2):
            kb, vb = k_ref[slot[p]], v_ref[slot[p]]
            keys[rows(p), :] = kb
            vals[rows(p), :] = vb
            keys_t[:, rows(p)] = kb.astype(F32).T.astype(BF16)
            vals_t[:, rows(p)] = vb.astype(F32).T.astype(BF16)
        if bwd:
            dk_ref[...] = jnp.zeros_like(dk_ref)
            dv_ref[...] = jnp.zeros_like(dv_ref)

    iota = functools.partial(lax.broadcasted_iota, jnp.int32, (SUB, SUB))
    causal = iota(0) <= iota(1)
    subs = range(N_SUB)
    tile = lambda j: slice(SUB * j, SUB * (j + 1))
    per = PIECE // SUB
    at = lambda i: (slot[i // per], tile(i % per))
    at_t = lambda i: (slot[i // per], slice(None), tile(i % per))
    base = lambda i, j: tile(i * (i + 1) // 2 + j)
    q = [q_ref[at(i)] for i in subs]
    d_o = [do_ref[at(i)] for i in subs] if bwd else None

    def score(i, j):
        s = dot_nt(keys[tile(j), :], q[i])
        return jnp.where(causal, s, -jnp.inf) if j == i else s

    top, inv, out_t = {}, {}, {}
    if fwd:
        for i in subs:
            for j in range(i + 1):
                s = score(i, j)
                s_buf[base(i, j), :] = s
                m = jnp.max(s, axis=0, keepdims=True)
                top[i] = m if j == 0 else jnp.maximum(top[i], m)
        for i in subs:
            for j in range(i + 1):
                p = jnp.exp(s_buf[base(i, j), :] - top[i])
                if bwd:
                    s_buf[base(i, j), :] = p
                part = jnp.sum(p, axis=0, keepdims=True)
                acc = dot_nn(vals_t[:, tile(j)], p.astype(BF16))
                total = part if j == 0 else total + part
                o_t = acc if j == 0 else o_t + acc
            inv[i] = 1.0 / total
            o_t = o_t * inv[i]
            out_t[i] = o_t.astype(BF16)
            o_ref[at(i)] = o_t.T.astype(BF16)
            if turned:
                t_ref[(slot[i // per], 0, slice(None), tile(i % per))] = out_t[i]
            if not bwd:
                ot_ref[at_t(i)] = out_t[i]
                lse_ref[:, tile(i)] = top[i] + jnp.log(total)
    if not bwd:
        return
    for i in subs:
        o_t = out_t[i] if fwd else ot_ref[at_t(i)]
        delta = jnp.sum(o_t.astype(F32) * d_o[i].astype(F32).T, axis=0, keepdims=True)
        for j in range(i + 1):
            p = s_buf[base(i, j), :] * inv[i] if fwd else jnp.exp(score(i, j) - lse_ref[:, tile(i)])
            dp = dot_nt(vals[tile(j), :], d_o[i])
            p_buf[tile(j), tile(i)] = p.astype(BF16)
            ds_buf[tile(j), tile(i)] = (p * (dp - delta)).astype(BF16)
    for i in subs:
        width = SUB * (i + 1)
        dq = dot_nn(keys_t[:, :width], ds_buf[:width, tile(i)]) * SCALE
        low, high, cos, sin = dq[:HALF], dq[HALF:], cos_ref[:, tile(i)], sin_ref[:, tile(i)]
        dq = stack([low * cos + high * sin, high * cos - low * sin])
        dq_ref[at(i)] = dq.T.astype(BF16)
        if turned:
            t_ref[(slot[i // per], 1, slice(None), tile(i % per))] = dq.astype(BF16)
    for j in subs:
        dv_ref[tile(j), :] += dot_nn(p_buf[tile(j), SUB * j :], stack(d_o[j:]))
        dk_ref[tile(j), :] += dot_nn(ds_buf[tile(j), SUB * j :], stack(q[j:]))


def attention(scal, mode, q, k, v, d_o=None, tables=(), saved=(), l0=0, turned=False):
    nl, _, n_heads = q.shape[:3]
    fwd, bwd = mode != "bwd", mode != "fwd"
    pick_head = lambda l, h, s: (l, 0, h)
    act = spec((None, 2, None, PIECE, E), pick_head)
    flat = spec((None, 2, None, E, PIECE), pick_head)
    kv_spec = spec((None, 2, PIECE, E), lambda l, h, s: (l + l0,))
    stat = spec((None, None, 1, ROWS), lambda l, h, s: (l, h))
    acc = spec((None, ROWS, E), lambda l, h, s: (l,))
    ins, specs, outs, out_specs = [q, k, v], [act, kv_spec, kv_spec], [], []
    act_shape = struct(BF16, nl, 2, n_heads, PIECE, E)
    if bwd:
        ins += [d_o, *tables]
        specs += [act] + [spec((HALF, ROWS))] * 2
    if not fwd:
        ins += saved
        specs += [flat, stat]
    if fwd:
        outs.append(act_shape)
        out_specs.append(act)
    if not bwd:
        outs += [struct(BF16, nl, 2, n_heads, E, PIECE), struct(F32, nl, n_heads, 1, ROWS)]
        out_specs += [flat, stat]
    if bwd:
        outs += [act_shape] + [struct(F32, nl, ROWS, E)] * 2
        out_specs += [act, acc, acc]
    if turned:
        outs.append(struct(BF16, nl, 2, n_heads, 2, E, PIECE))
        out_specs.append(spec((None, 2, None, 2, E, PIECE), pick_head))
    products = 2 * fwd + 4 * bwd + (not fwd)
    square = (ROWS, ROWS) if bwd else (SUB, SUB)
    return call(
        functools.partial(attn_body, mode, turned),
        (nl, n_heads),
        scal,
        ins,
        specs,
        outs,
        out_specs,
        nl * n_heads * products * 4 * E * SUB * SUB * N_TILE,
        scratch=[pltpu.VMEM((ROWS, E), BF16)] * 2
        + [pltpu.VMEM((E, ROWS), BF16)] * 2
        + [pltpu.VMEM((N_TILE * SUB if fwd else SUB, SUB), F32)]
        + [pltpu.VMEM(square, BF16)] * 2,
    )


def combine_body(kind, n_act, n_w, fresh, s_ref, *refs):
    acts, ws, refs = refs[:n_act], refs[n_act : n_act + n_w], refs[n_act + n_w :]
    c = s_ref[1]
    a = lanes([stack([r[0, h], r[1, h]]) for r in acts for h in range(r.shape[1])])
    pieces = [ws[0][pl.ds(GROUP * i, GROUP)] for i in (c, 1 - c)] + [w[...] for w in ws[1:]]
    if kind == "out":
        x = dot_nn(a, stack([w.reshape(w.shape[0] * E, w.shape[2]) for w in pieces]))
    else:
        x = dot_nt(a, lanes([w[h] for w in pieces for h in range(w.shape[0])] + [r[...] for r in refs[:2]]))
    x = x.astype(BF16)
    outs = refs[-3:] if fresh else refs[-2:]
    outs[0][...] = x[rows(0)]
    outs[1][...] = x[rows(1)]
    if fresh:
        outs[2][...] = x[rows(0)]


def combine(scal, kind, l, acts, ls, weights, kv=(), big=None):
    d = weights[0].shape[2 if kind == "out" else 1]
    in_specs = [
        spec((None, 2, a.shape[2], PIECE, E), lambda n, s, i=i: (i,)) for a, i in zip(acts, ls, strict=True)
    ]
    if kind == "out":
        in_specs += [spec((w.shape[0], E, COLS), lambda n, s: (0, 0, n)) for w in weights]
    else:
        in_specs += [spec((w.shape[0], COLS, E), lambda n, s: (0, n)) for w in weights]
        in_specs += [spec((COLS, E), lambda n, s: (n,))] * 2
    ins, aliases = [*acts, *weights, *kv], {}
    piece = spec((PIECE, COLS), lambda n, s: (0, n))
    fresh = big is None
    if not fresh:
        aliases = {1 + len(ins): 0}
        ins.append(big)
        in_specs.append(pl.BlockSpec(memory_space=pl.ANY))
    return call(
        functools.partial(combine_body, kind, len(acts), len(weights), fresh),
        (d // COLS,),
        scal,
        ins,
        in_specs,
        [struct(BF16, 8, PIECE, d)] + [struct(BF16, PIECE, d)] * (1 + fresh),
        [spec((None, PIECE, COLS), lambda n, s: (seq_of(l, s), 0, n))] + [piece] * (1 + fresh),
        2 * ROWS * sum(a.shape[2] for a in acts) * E * d,
        aliases=aliases,
    )


def dw_local_body(s_ref, t_ref, *refs):
    xs, o_ref = refs[:4], refs[4]
    a = lanes([stack([t_ref[l, p, h] for h in range(t_ref.shape[2])]) for l in range(2) for p in range(2)])
    o_ref[...] = dot_nn(a, stack([x[...] for x in xs])).reshape(o_ref.shape)


def dw_local(scal, which, turned, x, x_recv):
    d = x.shape[-1]
    block = (None, PIECE, DW_COLS)
    mine = [spec(block, lambda n, s, l=l: (seq_of(l, s), 0, n)) for l in range(2)]
    recv = [spec(block, lambda n, s, l=l: (l, 0, n)) for l in range(2)]
    n_heads = turned.shape[2]
    return call(
        dw_local_body,
        (d // DW_COLS,),
        scal,
        [turned, x, x_recv, x, x_recv],
        [spec((2, 2, n_heads, None, E, PIECE), lambda n, s: (0, 0, 0, which)), mine[0], recv[0], mine[1], recv[1]],
        struct(F32, n_heads, E, d),
        spec((n_heads, E, DW_COLS), lambda n, s: (0, 0, n)),
        4 * n_heads * E * ROWS * d,
    )


def dw_rest_body(n_t, last, flip, s_ref, *refs):
    ts, xs, refs = refs[:n_t], refs[n_t : n_t + 4], refs[n_t + 4 :]
    half = n_t // 4
    a = lanes([stack([t[h] for t in ts[half * g : half * (g + 1)] for h in range(UNIT)]) for g in range(4)])
    acc = dot_nn(a, stack([x[...] for x in xs])).reshape(GROUP, E, DW_COLS) + refs[0][...]
    if last:
        acc = acc + refs[1][...]
    outs = refs[-2:] if last else refs[-1:]
    for h in range(GROUP):
        x = acc[h].T if flip else acc[h]
        for o in outs:
            o[h] = x


def dw_rest(scal, which, half, turned, x, local, recv=None):
    d = x.shape[-1]
    last = recv is not None
    flip = last and which == 1
    specs = []
    for g, group in enumerate(turned):
        i = half ^ (g % 2)
        specs += [spec((UNIT, None, E, PIECE), lambda n, s, i=i: (i, which)) for _ in group]
    for g in range(4):
        seq = lambda s, g=g: 2 * jnp.bitwise_xor(s[0], 1 + g // 2) + jnp.bitwise_xor(s[1], g % 2)
        specs.append(spec((None, PIECE, DW_COLS), lambda n, s, seq=seq: (seq(s), 0, n)))
    block, at_n = (GROUP, E, DW_COLS), lambda n, s: (0, 0, n)
    specs += [spec(block, lambda n, s: (half, 0, n))]
    flat = [t for group in turned for t in group]
    ins = [*flat, x, x, x, x, local]
    outs, out_specs = [struct(F32, GROUP, E, d)], [spec(block, at_n)]
    if last:
        ins.append(recv)
        specs.append(spec(block, at_n))
        if flip:
            block = (GROUP, DW_COLS, E)
            outs = [struct(F32, n * GROUP, d, E) for n in (2, 1)]
            out_specs = [spec(block, lambda n, s: (s[1], n)), spec(block, lambda n, s: (0, n))]
        else:
            outs = [struct(F32, n * GROUP, E, d) for n in (2, 1)]
            out_specs = [spec(block, lambda n, s: (s[1], 0, n)), spec(block, at_n)]
    return call(
        functools.partial(dw_rest_body, len(flat), last, flip),
        (d // DW_COLS,),
        scal,
        ins,
        specs,
        outs,
        out_specs,
        4 * GROUP * E * ROWS * d,
    )


def copy_body(s_ref, x_ref, o_ref):
    o_ref[...] = x_ref[...]


def pick(indices, x, block):
    count, rest = indices.shape[0], x.shape[1:]
    return call(
        copy_body,
        (count,),
        indices,
        [x],
        [spec((block, *rest), lambda i, s: (s[i],))],
        struct(x.dtype, count * block, *rest),
        spec((block, *rest), lambda i, s: (i,)),
        x.size,
    )


def place_body(n, s_ref, *refs):
    for j in range(n):

        @pl.when(pl.program_id(0) == j)
        def _():
            refs[-1][...] = refs[j][...]


def place(seqs, big, pieces):
    n, d = len(pieces), big.shape[-1]
    return call(
        functools.partial(place_body, n),
        (n,),
        seqs,
        [*pieces, big],
        [spec((PIECE, d))] * n + [pl.BlockSpec(memory_space=pl.ANY)],
        struct(big.dtype, *big.shape),
        spec((None, PIECE, d), lambda i, s: (s[i],)),
        n * PIECE * d,
        aliases={1 + n: 0},
    )


def dkv_body(n, s_ref, *refs):
    acc = dot_nn(lanes([r[...].reshape(2 * E, PIECE) for r in refs[:n]]), stack([x[...] for x in refs[n:-2]]))
    for i, o in enumerate(refs[-2:]):
        o[...] = acc[E * i : E * (i + 1)].T


def d_w_kv(seqs, pieces, x):
    n, d = len(pieces), x.shape[-1]
    return call(
        functools.partial(dkv_body, n),
        (d // DW_COLS,),
        seqs,
        [*pieces] + [x] * n,
        [spec((2, E, PIECE))] * n
        + [spec((None, PIECE, DW_COLS), lambda i, s, j=j: (s[j], 0, i)) for j in range(n)],
        [struct(F32, d, E)] * 2,
        [spec((DW_COLS, E), lambda i, s: (i,))] * 2,
        4 * n * PIECE * E * d,
    )


def after(x, *deps):
    return lax.optimization_barrier((x, *deps))[0]


def solution(mesh):
    n_tp, n_cp = mesh.shape["tp"], mesh.shape["cp"]
    chips = range(n_tp)

    def on_chip(x):
        return lax.ppermute(x, "cp", [(c, n_cp - 1 - c) for c in range(n_cp)])

    def to_chip(x, flip):
        return lax.ppermute(x, "tp", [(i, i ^ flip) for i in chips])

    def to_chip_other(x, flip):
        pairs = [(i * n_cp + c, (i ^ flip) * n_cp + (1 - c)) for i in chips for c in range(n_cp)]
        return lax.ppermute(x, ("tp", "cp"), pairs)

    def spread(m, r):
        return [f(x, flip) for flip in (1, 2) for f, x in ((to_chip, m), (to_chip_other, r))] + [on_chip(r)]

    def swap_heads(x):
        return [
            f(x[0, p, GROUP * i : GROUP * (i + 1)], 1 + i)
            for i in range(2)
            for p, f in enumerate((to_chip, to_chip_other))
        ]

    def with_partner(ws):
        return [x for w in ws for x in (w, on_chip(w))]

    def relay(w_in, u, dep):
        ws = [after(w_in[a, u], dep) for a in (1, 2)]
        return with_partner(ws), to_chip(ws[u], 2 - u)

    def local_program(hidden, grad, w_query, w_key, w_value, w_out):
        t, c = lax.axis_index("tp"), lax.axis_index("cp")
        chain = [jnp.stack([t, c]).astype(jnp.int32)]

        def step(f, *args, **kw):
            out = f(chain[0], *args, **kw)
            chain[0] = after(chain[0], jax.tree.leaves(out)[0])
            return out

        cos, sin = rope_angles(ROWS)
        tables = lanes([cos, cos]), lanes([-sin, sin])
        tables_t = cos.T, sin.T
        wq, wo = w_query.transpose(1, 0, 2), w_out
        kv_w = (w_key, w_value)
        own, ext, nx, ny = 2 * t, 2 * (3 - t), 2 * (t ^ 1), 2 * (t ^ 2)
        theirs = jnp.stack([own + 1 - c, ext + 1 - c]).astype(jnp.int32)
        unit = lambda u: (2 * c + u).astype(jnp.int32)[None]

        wq_in, wo_in = {}, {}
        sent = pick(unit(0), wq, UNIT)
        for a in (1, 2):
            wq_in[a, 0] = to_chip(sent, a)
        sent = pick(after(theirs, sent), hidden, 1)
        h_recv = on_chip(sent)
        sent = pick(after(unit(0), sent), wo, UNIT)
        for a in (1, 2):
            wo_in[a, 0] = to_chip(sent, a)
        sent = pick(after(theirs, sent), grad, 1)
        g_recv = on_chip(sent)

        k, v, q_0 = step(proj, "q", hidden, h_recv, [wq], tables, kv=kv_w)
        sent_q = pick(after(unit(1), q_0), wq, UNIT)
        sent_o = pick(after(unit(1), sent_q), wo, UNIT)
        for w_in, sent in ((wq_in, sent_q), (wo_in, sent_o)):
            for a in (1, 2):
                w_in[a, 1] = to_chip(sent, a)
        chain[0] = after(chain[0], sent_o)
        (do_0,) = step(proj, "do", grad, g_recv, [wo])
        wq_n0, wq_d0 = relay(wq_in, 0, do_0)
        o_0, dq_0, dk_0, dv_0, t_0 = step(attention, "fused", q_0, k, v, do_0, tables_t, turned=True)
        dwo = step(dw_local, 0, t_0, grad, g_recv)

        wo_n0, wo_d0 = relay(wo_in, 0, dwo)
        (q_n0,) = step(proj, "q", hidden, h_recv, wq_n0, tables)
        (do_n0,) = step(proj, "do", grad, g_recv, wo_n0)
        wq_n1, wq_d1 = relay(wq_in, 1, do_n0)
        o_n0, dq_n0, dk_n0, dv_n0, t_n0 = step(attention, "fused", q_n0, k, v, do_n0, tables_t, turned=True)
        dwq = step(dw_local, 1, t_0, hidden, h_recv)
        wo_n1, wo_d1 = relay(wo_in, 1, dwq)
        (q_n1,) = step(proj, "q", hidden, h_recv, wq_n1, tables)
        (do_n1,) = step(proj, "do", grad, g_recv, wo_n1)
        t_nb0 = swap_heads(after(t_n0, do_n1))
        wq_d = with_partner([after(w, do_n1) for w in (wq_d0, wq_d1)])
        o_n1, dq_n1, dk_n1, dv_n1, t_n1 = step(attention, "fused", q_n1, k, v, do_n1, tables_t, turned=True)
        t_nb1 = swap_heads(t_n1)
        t_nb = list(zip(t_nb0, t_nb1, strict=True))

        wo_d = with_partner([after(w, o_n1) for w in (wo_d0, wo_d1)])
        wo_all = [wo, *wo_n0, *wo_n1, *wo_d]
        wq_all = [wq, *wq_n0, *wq_n1, *wq_d]
        (q_d,) = step(proj, "q", hidden, h_recv, wq_d, tables, nl=1)
        o_d, ot_d, lse_d = step(attention, "fwd", q_d, k, v)
        out_big, out_r, out_m = step(combine, "out", 0, [o_0, o_n0, o_n1, o_d], [0] * 4, wo_all)
        out_in = spread(out_m, out_r)
        (do_d,) = step(proj, "do", grad, g_recv, wo_d, nl=1)
        dq_d, dk_d, dv_d = step(attention, "bwd", q_d, k, v, do_d, tables_t, saved=[ot_d, lse_d])

        def finish_kv(l, *last):
            dk, dv = [
                x[l] + y[l] + z[l] + w[0]
                for x, y, z, w in zip((dk_0, dv_0), (dk_n0, dv_n0), (dk_n1, dv_n1), last, strict=True)
            ]
            dk = dk * tables[0] - jnp.roll(dk, HALF, axis=1) * tables[1]
            x = jnp.stack([dk, dv]).astype(BF16).reshape(2, 2, PIECE, E).transpose(1, 0, 2, 3)
            x = jnp.where(c == 0, x, x[::-1])
            return x[None], x.transpose(0, 1, 3, 2)

        dkv_0, dkv_t = finish_kv(0, dk_d, dv_d)
        dkv_in = spread(dkv_t[0], dkv_t[1])
        dh_big, dh_r, dh_m = step(combine, "dh", 0, [dq_0, dq_n0, dq_n1, dq_d, dkv_0], [0] * 5, wq_all, kv=kv_w)
        dh_in = spread(dh_m, dh_r)

        (q_e,) = step(proj, "q", hidden, h_recv, wq_d, tables, l0=1, nl=1)
        (do_e,) = step(proj, "do", grad, g_recv, wo_d, l0=1, nl=1)
        o_e, dq_e, dk_e, dv_e = step(attention, "fused", q_e, k, v, do_e, tables_t, l0=1)
        dkv_1, dkv_u = finish_kv(1, dk_e, dv_e)
        dkv_in.append(on_chip(dkv_u[1]))

        (wo_part,) = step(dw_rest, 0, 1, t_nb, grad, dwo)
        wo_part = on_chip(wo_part)
        (wq_part,) = step(dw_rest, 1, 1, t_nb, hidden, dwq)
        wq_part = on_chip(wq_part)
        out_big, out_er = step(combine, "out", 1, [o_0, o_n0, o_n1, o_e], [1, 1, 1, 0], wo_all, big=out_big)
        out_in.append(on_chip(out_er))
        dwo_big, dwo_mine = step(dw_rest, 0, 0, t_nb, grad, dwo, wo_part)
        dwo_theirs = on_chip(dwo_mine)
        dwq_big, dwq_mine = step(dw_rest, 1, 0, t_nb, hidden, dwq, wq_part)
        dwq_theirs = on_chip(dwq_mine)
        dh_big, dh_er = step(
            combine, "dh", 1, [dq_0, dq_n0, dq_n1, dq_e, dkv_1], [1, 1, 1, 0, 0], wq_all, kv=kv_w, big=dh_big
        )
        dh_in.append(on_chip(dh_er))

        seqs = [nx + c, nx + 1 - c, ny + c, ny + 1 - c, own + 1 - c, ext + 1 - c]
        put = lambda big, x: lax.dynamic_update_slice_in_dim(big, x, GROUP * (1 - c), 0)
        places = jnp.stack([*seqs, own + c, ext + c]).astype(jnp.int32)
        attn_out = place(after(places, dh_er), out_big, out_in)
        d_kv = d_w_kv(after(places, attn_out), [*dkv_in, dkv_t[0], dkv_u[0]], hidden)
        d_w_key, d_w_value = [x + on_chip(x) for x in d_kv]
        d_w_out = put(dwo_big, dwo_theirs)
        d_w_query = put(dwq_big, dwq_theirs).transpose(1, 0, 2)
        d_hidden = place(after(places, d_kv[0]), dh_big, dh_in)
        return attn_out, d_hidden, d_w_query, d_w_key, d_w_value, d_w_out

    row = P(None, "cp", None)
    wq_spec, wo_spec = P(None, "tp", None), P("tp", None, None)
    return jax.shard_map(
        local_program,
        mesh=mesh,
        in_specs=(row, row, wq_spec, P(), P(), wo_spec),
        out_specs=(row, row, wq_spec, P(), P(), wo_spec),
        check_vma=False,
    )
```

```python
import functools

import jax
import jax.numpy as jnp
from jax import lax
from jax.experimental import pallas as pl
from jax.experimental.pallas import tpu as pltpu
from jax.sharding import PartitionSpec as P


F32 = jnp.float32
BF16 = jnp.bfloat16
ROPE_BASE = 10000.0
VMEM_LIMIT = 67043328
PIECE = 512
SUB = 256
E = 128
HALF = E // 2
ROWS = 2 * PIECE
N_SUB = ROWS // SUB
N_TILE = N_SUB * (N_SUB + 1) // 2
GROUP = 6
UNIT = 3
WIDE = GROUP * E
COLS = 512
DW_COLS = 1024
SCALE = E**-0.5
OWN = "own"
ALL = slice(None)
HBM = pl.BlockSpec(memory_space=pl.ANY)


def rope_angles(n_pos):
    inv_freq = 1.0 / jnp.power(ROPE_BASE, jnp.arange(HALF, dtype=F32) * (2.0 / E))
    angles = jnp.arange(n_pos).astype(F32)[:, None] * inv_freq[None, :]
    return jnp.cos(angles), jnp.sin(angles)


def dot_nn(a, b):
    return jnp.dot(a, b, preferred_element_type=F32)


def dot_nt(a, b):
    return lax.dot_general(a, b, (((1,), (1,)), ((), ())), preferred_element_type=F32)


def lanes(parts):
    return jnp.concatenate(parts, axis=1)


def stack(parts):
    return jnp.concatenate(parts, axis=0)


def rows(p):
    return slice(PIECE * p, PIECE * (p + 1))


def heads(e):
    return slice(E * e, E * (e + 1))


def spec(block, index=None, once=False):
    rank = len(block)

    def full(*a):
        i = tuple(index(*a)) if index else ()
        return i + (0,) * (rank - len(i))

    mode = {"pipeline_mode": pl.Buffered(1)} if once or not index else {}
    return pl.BlockSpec(block, full, **mode)


def struct(dtype, *shape):
    return jax.ShapeDtypeStruct(shape, dtype)


def call(body, grid, scal, ins, in_specs, outs, out_specs, flops, scratch=(), aliases=None):
    nbytes = sum(x.size * x.dtype.itemsize for x in jax.tree.leaves([ins, outs]))
    return pl.pallas_call(
        body,
        grid_spec=pltpu.PrefetchScalarGridSpec(
            num_scalar_prefetch=1, grid=grid, in_specs=in_specs, out_specs=out_specs, scratch_shapes=scratch
        ),
        out_shape=outs,
        input_output_aliases=aliases or {},
        cost_estimate=pl.CostEstimate(flops=int(flops), bytes_accessed=int(nbytes), transcendentals=0),
        compiler_params=pltpu.CompilerParams(vmem_limit_bytes=VMEM_LIMIT),
    )(scal, *ins)


def seq_of(l, s):
    return 2 * jnp.where(l == 0, s[0], 3 - s[0]) + s[1]


def proj_body(kind, n_w, n_kv, steps, nl, s_ref, x_ref, r_ref, *refs):
    queries = kind == "q"
    if queries:
        cos_ref, sin_ref, *refs = refs
    w_refs, kv_refs, refs = refs[:n_w], refs[n_w : n_w + n_kv], refs[n_w + n_kv :]
    *outs, a_buf, w_buf, kv_buf, a_sem, w_sem, kv_sem = refs
    l, n = pl.program_id(0), pl.program_id(1)
    c = s_ref[1]
    per = n_w // steps if n_w > 1 else 1
    size = GROUP // per

    def row_copies(i):
        parts = (x_ref, seq_of(i, s_ref)), (r_ref, i)
        return [pltpu.make_async_copy(x.at[at], a_buf.at[i, p], a_sem.at[i, p]) for p, (x, at) in enumerate(parts)]

    def weight_copies(j):
        copies = []
        for m in range(per):
            src = w_refs[per * j + m] if n_w > 1 else w_refs[0].at[pl.ds(GROUP * jnp.bitwise_xor(j, c), GROUP)]
            copies.append(pltpu.make_async_copy(src, w_buf.at[pl.ds(GROUP * j + size * m, size)], w_sem.at[j, m]))
        return copies

    def kv_copies():
        return [pltpu.make_async_copy(r, kv_buf.at[i], kv_sem.at[i]) for i, r in enumerate(kv_refs)]

    def at_step(i, j, f, copies):
        @pl.when(jnp.logical_and(l == i, n == j))
        def _():
            for copy in copies():
                getattr(copy, f)()

    def product(ws):
        return dot_nn(stack([a_buf[l, p] for p in range(2)]), lanes(ws))

    def rotated(x, p):
        at = pl.ds(pl.multiple_of(PIECE * jnp.bitwise_xor(p, c), PIECE), PIECE)
        return x * cos_ref[at, :] + pltpu.roll(x, HALF, 1) * sin_ref[at, :]

    everything = lambda: sum(
        [row_copies(0), *map(weight_copies, range(steps)), kv_copies(), *map(row_copies, range(1, nl))], []
    )
    at_step(0, 0, "start", everything)
    for i in range(nl):
        at_step(i, 0, "wait", functools.partial(row_copies, i))
    for j in range(steps):
        at_step(0, j, "wait", functools.partial(weight_copies, j))

    @pl.when(n < steps)
    def _():
        if queries:
            x = product([w_buf[GROUP * n + e] for e in range(GROUP)])
        else:
            w = w_buf[pl.ds(GROUP * n, GROUP)]
            x = dot_nt(stack([a_buf[l, p] for p in range(2)]), w.reshape(WIDE, w.shape[2]))
        for p in range(2):
            for e in range(GROUP):
                part = x[rows(p), heads(e)]
                outs[-1][p, e] = (rotated(part, p) * SCALE if queries else part).astype(BF16)

    if n_kv:
        at_step(0, steps, "wait", kv_copies)

        @pl.when(n == steps)
        def _():
            x = product([kv_buf[i] for i in range(n_kv)])
            for p in range(2):
                outs[0][p] = rotated(x[rows(p), :E], p).astype(BF16)
                outs[1][p] = x[rows(p), E:].astype(BF16)


def proj(scal, kind, x, x_recv, weights, tables=(), kv=(), nl=2):
    d = x.shape[-1]
    steps = 2 if len(weights) == 1 else len(weights) // 2
    shape = (d, E) if kind == "q" else (E, d)
    dma = pltpu.SemaphoreType.DMA
    last = steps - 1
    return call(
        functools.partial(proj_body, kind, len(weights), len(kv), steps, nl),
        (nl, steps + len(kv) // 2),
        scal,
        [x, x_recv, *tables, *weights, *kv],
        [HBM] * 2 + [spec((ROWS, E))] * len(tables) + [HBM] * (len(weights) + len(kv)),
        [struct(BF16, nl, 2, PIECE, E)] * len(kv) + [struct(BF16, nl, 2, steps * GROUP, PIECE, E)],
        [spec((None, 2, PIECE, E), lambda l, n, s: (l,))] * len(kv)
        + [spec((None, 2, GROUP, PIECE, E), lambda l, n, s: (l, 0, jnp.minimum(n, last)))],
        2 * nl * ROWS * d * steps * WIDE,
        scratch=[
            pltpu.VMEM((nl, 2, PIECE, d), BF16),
            pltpu.VMEM((steps * GROUP, *shape), BF16),
            pltpu.VMEM((len(kv) or 1, d if kv else GROUP, E), BF16),
            dma((nl, 2)),
            dma((steps, 2)),
            dma((2,)),
        ],
    )


TRIO = 3


def over_keys(f, x):
    return f(x, axis=0, keepdims=True)


PART = 32


def weave(*lists):
    order = sorted((i / len(fs), j, f) for j, fs in enumerate(lists) for i, f in enumerate(fs))
    for _, _, f in order:
        f()


def attn_body(mode, turned, joined, s_ref, *refs):
    it = iter(refs)
    fwd, bwd = mode != "bwd", mode != "fwd"
    q_ref, k_ref, v_ref = next(it), next(it), next(it)
    if bwd:
        do_ref, cos_ref, sin_ref = next(it), next(it), next(it)
    if not fwd:
        ot_ref, lse_ref = next(it), next(it)
    if joined:
        next(it)
    if fwd:
        o_ref = next(it)
    if not bwd:
        ot_ref, lse_ref = next(it), next(it)
    if bwd:
        dq_ref, dk_ref, dv_ref = next(it), next(it), next(it)
    if turned:
        t_ref = next(it)
    keys, vals, keys_t, vals_t, s_bufs, p_buf, ds_buf = it
    slot = [jnp.bitwise_xor(p, s_ref[1]) for p in range(2)]

    @pl.when(pl.program_id(1) == 0)
    def _():
        for p in range(2):
            kb, vb = k_ref[slot[p]], v_ref[slot[p]]
            keys[rows(p), :] = kb
            vals[rows(p), :] = vb
            keys_t[:, rows(p)] = kb.astype(F32).T.astype(BF16)
            vals_t[:, rows(p)] = vb.astype(F32).T.astype(BF16)
        if bwd:
            dk_ref[...] = jnp.zeros_like(dk_ref)
            dv_ref[...] = jnp.zeros_like(dv_ref)

    iota = functools.partial(lax.broadcasted_iota, jnp.int32, (SUB, SUB))
    causal = iota(0) <= iota(1)
    subs = range(N_SUB)
    tiles = [(i, j) for i in subs for j in range(i + 1)]
    tile = lambda j: slice(SUB * j, SUB * (j + 1))
    per = PIECE // SUB
    base = lambda i, j: tile(i * (i + 1) // 2 + j)
    here = lambda i, h: (slot[i // per], h)
    q = [[q_ref[(*here(i, h), tile(i % per))] for i in subs] for h in range(TRIO)]
    d_o = [[do_ref[(*here(i, h), tile(i % per))] for i in subs] for h in range(TRIO)] if bwd else None

    def phases(h):
        top, inv, total, out_t, delta = {}, {}, {}, {}, {}
        s_buf = s_bufs.at[h]

        def score(i, j):
            s = dot_nt(keys[tile(j), :], q[h][i])
            return jnp.where(causal, s, -jnp.inf) if j == i else s

        def add(sums, i, first, x, f):
            sums[i] = x if first else f(sums[i], x)

        def fold(x, f):
            return f(x.reshape(PART // 8, 8, SUB), axis=0)

        def parts(i, j):
            start = base(i, j).start
            return [(slice(PART * r, PART * (r + 1)), slice(start + PART * r, start + PART * (r + 1))) for r in range(SUB // PART)]

        def scores(i, j):
            s = score(i, j)
            for r, at in parts(i, j):
                s_buf[at, :] = s[r]
                add(top, i, j == 0 and r.start == 0, fold(s[r], jnp.max), jnp.maximum)
            if j == i:
                top[i] = over_keys(jnp.max, top[i])

        def weights(i, j):
            for r, at in parts(i, j):
                p = jnp.exp(s_buf[at, :] - top[i])
                if bwd:
                    s_buf[at, :] = p
                add(total, i, j == 0 and r.start == 0, fold(p, jnp.sum), jnp.add)
                p_buf[h, SUB * j + r.start : SUB * j + r.stop, tile(i)] = p.astype(BF16)
            if j == i:
                width = SUB * (i + 1)
                total[i] = over_keys(jnp.sum, total[i])
                inv[i] = 1.0 / total[i]
                o_t = dot_nn(vals_t[:, :width], p_buf[h, :width, tile(i)]) * inv[i]
                out_t[i] = o_t.astype(BF16)
                o_ref[(*here(i, h), tile(i % per))] = o_t.T.astype(BF16)
                if turned:
                    t_ref[(*here(i, h), 0, ALL, tile(i % per))] = out_t[i]
                if not bwd:
                    ot_ref[(*here(i, h), ALL, tile(i % per))] = out_t[i]
                    lse_ref[h, :, tile(i)] = top[i] + jnp.log(total[i])

        def score_grads(i, j):
            if j == 0:
                o_t = out_t[i] if fwd else ot_ref[(*here(i, h), ALL, tile(i % per))]
                delta[i] = over_keys(jnp.sum, o_t.astype(F32) * d_o[h][i].astype(F32).T)
            s = None if fwd else score(i, j)
            dp = dot_nt(vals[tile(j), :], d_o[h][i])
            for r, at in parts(i, j):
                p = s_buf[at, :] * inv[i] if fwd else jnp.exp(s[r] - lse_ref[h, :, tile(i)])
                to = slice(SUB * j + r.start, SUB * j + r.stop)
                p_buf[h, to, tile(i)] = p.astype(BF16)
                ds_buf[h, to, tile(i)] = (p * (dp[r] - delta[i])).astype(BF16)

        def query_grads(i):
            width = SUB * (i + 1)
            dq = dot_nn(keys_t[:, :width], ds_buf[h, :width, tile(i)]) * SCALE
            low, high, cos, sin = dq[:HALF], dq[HALF:], cos_ref[:, tile(i)], sin_ref[:, tile(i)]
            dq = stack([low * cos + high * sin, high * cos - low * sin])
            dq_ref[(*here(i, h), tile(i % per))] = dq.T.astype(BF16)
            if turned:
                t_ref[(*here(i, h), 1, ALL, tile(i % per))] = dq.astype(BF16)

        def key_grads(j):
            dv_ref[tile(j), :] += dot_nn(p_buf[h, tile(j), SUB * j :], stack(d_o[h][j:]))
            dk_ref[tile(j), :] += dot_nn(ds_buf[h, tile(j), SUB * j :], stack(q[h][j:]))

        each = lambda f, some: [functools.partial(f, *x) for x in some]
        lists = [each(scores, tiles), each(weights, tiles)] if fwd else []
        if bwd:
            alone = [(i,) for i in subs]
            lists += [each(score_grads, tiles), each(query_grads, alone) + each(key_grads, alone)]
        return lists

    work = [phases(h) for h in range(TRIO)]
    n_phases = len(work[0])
    for stage in range(TRIO + n_phases - 1):
        weave(*(work[h][stage - h] for h in range(TRIO) if 0 <= stage - h < n_phases))


def attention(scal, mode, q, k, v, d_o=None, tables=(), saved=(), l0=0, nl=2, turned=None, prior=()):
    n_heads = q.shape[2]
    fwd, bwd = mode != "bwd", mode != "fwd"
    at_in, at_out = lambda l, h, s: (l + l0, 0, h), lambda l, h, s: (l, 0, h)
    block = (None, 2, TRIO, PIECE, E)
    act_in, act = spec(block, at_in), spec(block, at_out)
    flat = spec((None, 2, TRIO, E, PIECE), at_out)
    kv_spec = spec((None, 2, PIECE, E), lambda l, h, s: (l + l0,))
    stat = spec((None, TRIO, 1, ROWS), lambda l, h, s: (l, h))
    acc = spec((None, ROWS, E), lambda l, h, s: (l,))
    ins, specs, outs, out_specs = [q, k, v], [act_in, kv_spec, kv_spec], [], []
    act_shape = struct(BF16, nl, 2, n_heads, PIECE, E)
    if bwd:
        ins += [d_o, *tables]
        specs += [act_in] + [spec((HALF, ROWS))] * 2
    if not fwd:
        ins += saved
        specs += [flat, stat]
    if fwd:
        outs.append(act_shape)
        out_specs.append(act)
    if not bwd:
        outs += [struct(BF16, nl, 2, n_heads, E, PIECE), struct(F32, nl, n_heads, 1, ROWS)]
        out_specs += [flat, stat]
    if bwd:
        outs += [act_shape] + [struct(F32, nl, ROWS, E)] * 2
        out_specs += [act, acc, acc]
    if turned is not None:
        per = GROUP // TRIO
        shift = 0 if turned == OWN else per
        outs.append(struct(BF16, nl, 2, n_heads * (2 if shift else 1), 2, E, PIECE))
        place_head = lambda l, h, s: (l, 0, h + (per * (h // per + turned) if shift else 0))
        out_specs.append(spec((None, 2, TRIO, 2, E, PIECE), place_head))
    aliases = {1 + len(ins): len(outs) - 1} if prior else {}
    ins += prior
    specs += [HBM] * len(prior)
    products = 2 * fwd + 4 * bwd + (not fwd)
    square = TRIO, ROWS, ROWS
    return call(
        functools.partial(attn_body, mode, turned is not None, len(prior)),
        (nl, n_heads // TRIO),
        scal,
        ins,
        specs,
        outs,
        out_specs,
        nl * n_heads * products * 4 * E * SUB * SUB * N_TILE,
        scratch=[pltpu.VMEM((ROWS, E), BF16)] * 2
        + [pltpu.VMEM((E, ROWS), BF16)] * 2
        + [pltpu.VMEM((TRIO, N_TILE * SUB if fwd else SUB, SUB), F32)]
        + [pltpu.VMEM(square, BF16)] * 2,
        aliases=aliases,
    )


def in_flight(n, steps, chunks, buf, sem):
    slots = buf.shape[0]
    per = slots // 2

    def load(i):
        return pltpu.make_async_copy(chunks[i][0], buf.at[i % slots], sem.at[0, i % slots])

    def save(i):
        return pltpu.make_async_copy(buf.at[i % slots], chunks[i][1], sem.at[1, i % slots])

    for m in range(steps):

        @pl.when(n == m)
        def _():
            for i in range(max(per * (m - 1), 0), min(per * m, len(chunks))):
                load(i).wait()
                save(i).start()
            for i in range(per * m, min(per * (m + 1), len(chunks))):
                if i >= slots:
                    save(i - slots).wait()
                load(i).start()

    def finish():
        @pl.when(n == steps - 1)
        def _():
            for i in range(max(len(chunks) - slots, 0), len(chunks)):
                save(i).wait()

    return finish


def seq_near(s, flip, other):
    return 2 * jnp.bitwise_xor(s[0], flip) + jnp.bitwise_xor(s[1], other)


def combine_body(kind, n_act, n_w, near, fresh, steps, s_ref, *refs):
    acts, ws, refs = refs[:n_act], refs[n_act : n_act + n_w], refs[n_act + n_w :]
    c, n = s_ref[1], pl.program_id(0)
    if kind == "dh":
        kv_refs, refs = refs[:2], refs[2:]
    if not fresh:
        refs = refs[1:]
    finish = []
    if near:
        pieces, theirs, refs = refs[2 : 2 + len(near)], refs[2 + len(near)], refs[len(near) + 3 :]
        *refs, rows_out, grad_out, row_buf, grad_buf, row_sem, grad_sem = refs
        row_chunks = [
            (r.at[cut], rows_out.at[seq_near(s_ref, *at), cut])
            for r, at in zip(pieces, near, strict=True)
            for cut in (pl.ds(SUB * i, SUB) for i in range(PIECE // SUB))
        ]
        grad_chunks = [(theirs.at[i], grad_out.at[GROUP * (1 - c) + i]) for i in range(GROUP)]
        finish.append(in_flight(n, steps, row_chunks, row_buf, row_sem))
        finish.append(in_flight(n, steps, grad_chunks, grad_buf, grad_sem))
    a = lanes([stack([r[0, h], r[1, h]]) for r in acts for h in range(r.shape[1])])
    held = [ws[0][pl.ds(GROUP * i, GROUP)] for i in (c, 1 - c)] + [w[...] for w in ws[1:]]
    if kind == "out":
        x = dot_nn(a, stack([w.reshape(w.shape[0] * E, w.shape[2]) for w in held]))
    else:
        x = dot_nt(a, lanes([w[h] for w in held for h in range(w.shape[0])] + [r[...] for r in kv_refs]))
    x = x.astype(BF16)
    refs[0][...] = x[rows(0)]
    refs[1][...] = x[rows(1)]
    if fresh:
        refs[2][...] = x[rows(0)]
    for f in finish:
        f()


def combine(scal, kind, l, acts, ls, weights, kv=(), big=None, side=None):
    d = weights[0].shape[2 if kind == "out" else 1]
    steps = d // COLS
    in_specs = [
        spec((None, 2, a.shape[2], PIECE, E), lambda n, s, i=i: (i,), once=True) for a, i in zip(acts, ls, strict=True)
    ]
    if kind == "out":
        in_specs += [spec((w.shape[0], E, COLS), lambda n, s: (0, 0, n)) for w in weights]
    else:
        in_specs += [spec((w.shape[0], COLS, E), lambda n, s: (0, n)) for w in weights]
        in_specs += [spec((COLS, E), lambda n, s: (n,))] * 2
    piece = spec((PIECE, COLS), lambda n, s: (0, n))
    fresh = big is None
    ins, aliases, scratch, near = [*acts, *weights, *kv], {}, [], ()
    outs = [struct(BF16, 8, PIECE, d)] + [struct(BF16, PIECE, d)] * (1 + fresh)
    out_specs = [spec((None, PIECE, COLS), lambda n, s: (seq_of(l, s), 0, n))] + [piece] * (1 + fresh)
    moved = [] if fresh else [big]
    if side:
        whole, pieces, near, grad, theirs = side
        moved += [whole, grad, *pieces, theirs]
        outs += [struct(x.dtype, *x.shape) for x in (whole, grad)]
        out_specs += [HBM] * 2
        dma = pltpu.SemaphoreType.DMA
        scratch = [
            pltpu.VMEM((4, SUB, d), BF16),
            pltpu.VMEM((2, *theirs.shape[1:]), F32),
            dma((2, 4)),
            dma((2, 2)),
        ]
    for i, o in zip(range(3 if side else len(moved)), (0, 2, 3), strict=False):
        aliases[1 + len(ins) + i] = o
    return call(
        functools.partial(combine_body, kind, len(acts), len(weights), near, fresh, steps),
        (steps,),
        scal,
        ins + moved,
        in_specs + [HBM] * len(moved),
        outs,
        out_specs,
        2 * ROWS * sum(a.shape[2] for a in acts) * E * d,
        scratch=scratch,
        aliases=aliases,
    )


def dw_local_body(s_ref, t_ref, *refs):
    xs, o_ref = refs[:4], refs[4]
    a = lanes([stack([t_ref[l, p, h] for h in range(t_ref.shape[2])]) for l in range(2) for p in range(2)])
    o_ref[...] = dot_nn(a, stack([x[...] for x in xs])).reshape(o_ref.shape)


def dw_local(scal, which, turned, x, x_recv):
    d = x.shape[-1]
    block = (None, PIECE, DW_COLS)
    mine = [spec(block, lambda n, s, l=l: (seq_of(l, s), 0, n)) for l in range(2)]
    recv = [spec(block, lambda n, s, l=l: (l, 0, n)) for l in range(2)]
    n_heads = turned.shape[2]
    return call(
        dw_local_body,
        (d // DW_COLS,),
        scal,
        [turned, x, x_recv, x, x_recv],
        [spec((2, 2, n_heads, None, E, PIECE), lambda n, s: (0, 0, 0, which)), mine[0], recv[0], mine[1], recv[1]],
        struct(F32, n_heads, E, d),
        spec((n_heads, E, DW_COLS), lambda n, s: (0, 0, n)),
        4 * n_heads * E * ROWS * d,
    )


def dw_rest_body(last, s_ref, *refs):
    ts, xs, refs = refs[:8], refs[8:12], refs[12:]
    a = lanes([stack([t[h] for t in ts[2 * g : 2 * g + 2] for h in range(UNIT)]) for g in range(4)])
    acc = dot_nn(a, stack([x[...] for x in xs])).reshape(GROUP, E, DW_COLS) + refs[0][...]
    if last:
        acc = acc + refs[1][...]
    for o in refs[-2:] if last else refs[-1:]:
        o[...] = acc


NEAR = ((1, 0), (2, 0), (1, 1), (2, 1))


def near_specs(half, which):
    specs = []
    for _, other in NEAR:
        i = half ^ other
        specs += [spec((UNIT, None, E, PIECE), lambda n, s, j=j: (j, which)) for j in (i, 2 + i)]
    rows_at = [spec((None, PIECE, DW_COLS), lambda n, s, at=at: (seq_near(s, *at), 0, n)) for at in NEAR]
    return specs, rows_at


def dw_rest(scal, half, turned, x, local, recv=None):
    d = x.shape[-1]
    block, at_n = (GROUP, E, DW_COLS), lambda n, s: (0, 0, n)
    specs, rows_at = near_specs(half, 0)
    specs += rows_at + [spec(block, lambda n, s: (half, 0, n))]
    ins = [*(t for t in turned for _ in range(2)), x, x, x, x, local]
    outs, out_specs = [struct(F32, GROUP, E, d)], [spec(block, at_n)]
    last = recv is not None
    if last:
        ins.append(recv)
        specs.append(spec(block, at_n))
        outs.insert(0, struct(F32, 2 * GROUP, E, d))
        out_specs.insert(0, spec(block, lambda n, s: (s[1], 0, n)))
    return call(
        functools.partial(dw_rest_body, last),
        (d // DW_COLS,),
        scal,
        ins,
        specs,
        outs,
        out_specs,
        4 * GROUP * E * ROWS * d,
    )


def dw_in_body(last, s_ref, t_ref, u0_ref, u1_ref, *refs):
    ts, kvs, xs, refs = refs[:8], refs[8:12], refs[12:20], refs[20:]
    groups = [
        stack([t_ref[l, p, h] for h in range(GROUP)] + [u[p]]) for l, u in enumerate((u0_ref, u1_ref)) for p in range(2)
    ]
    groups += [
        stack([t[h] for t in ts[2 * g : 2 * g + 2] for h in range(UNIT)] + [kvs[g][...]]) for g in range(len(kvs))
    ]
    acc = dot_nn(lanes(groups), stack([x[...] for x in xs])).reshape(GROUP + 1, E, DW_COLS)
    if not last:
        refs[0][...] = acc
        return
    acc = acc + refs[0][...]
    for h in range(GROUP):
        refs[1][h] = refs[2][h] = acc[h].T
    refs[3][...] = acc[GROUP].T


def dw_in(scal, half, turned_0, kv_0, kv_1, turned, kv, x, x_recv, recv=None):
    d = x.shape[-1]
    kv_half = lambda s: jnp.bitwise_xor(half, s[1])
    near, rows_at = near_specs(half, 1)
    local = [spec((2, 2, GROUP, None, E, PIECE), lambda n, s: (0, 0, half, 1))]
    local += [spec((2, None, E, PIECE), lambda n, s: (0, kv_half(s)))] * 2
    block = (None, PIECE, DW_COLS)
    for l in range(2):
        rows_at.insert(2 * l, spec(block, lambda n, s, l=l: (seq_of(l, s), 0, n)))
        rows_at.insert(2 * l + 1, spec(block, lambda n, s, l=l: (l, 0, n)))
    near += [spec((None, E, PIECE), lambda n, s: (kv_half(s),))] * len(kv)
    ins = [turned_0, kv_0, kv_1, *(t for t in turned for _ in range(2)), *kv, x, x_recv, x, x_recv, x, x, x, x]
    specs = local + near + rows_at
    part = spec((GROUP + 1, E, DW_COLS), lambda n, s: (0, 0, n))
    outs, out_specs = [struct(F32, GROUP + 1, E, d)], [part]
    last = recv is not None
    if last:
        ins.append(recv)
        specs.append(part)
        block = (GROUP, DW_COLS, E)
        outs = [struct(F32, 2 * GROUP, d, E), struct(F32, GROUP, d, E), struct(F32, d, E)]
        out_specs = [spec(block, lambda n, s: (s[1], n)), spec(block, lambda n, s: (0, n))]
        out_specs.append(spec((DW_COLS, E), lambda n, s: (n,)))
    return call(
        functools.partial(dw_in_body, last),
        (d // DW_COLS,),
        scal,
        ins,
        specs,
        outs,
        out_specs,
        8 * (GROUP + 1) * E * ROWS * d,
    )


def copy_body(s_ref, x_ref, o_ref):
    o_ref[...] = x_ref[...]


def pick(indices, x, block):
    count, rest = indices.shape[0], x.shape[1:]
    return call(
        copy_body,
        (count,),
        indices,
        [x],
        [spec((block, *rest), lambda i, s: (s[i],))],
        struct(x.dtype, count * block, *rest),
        spec((block, *rest), lambda i, s: (i,)),
        x.size,
    )


def place_body(n, s_ref, *refs):
    for j in range(n):

        @pl.when(pl.program_id(0) == j)
        def _():
            refs[-1][...] = refs[j][...]


def place(seqs, big, pieces):
    n, d = len(pieces), big.shape[-1]
    return call(
        functools.partial(place_body, n),
        (n,),
        seqs,
        [*pieces, big],
        [spec((PIECE, d))] * n + [HBM],
        struct(big.dtype, *big.shape),
        spec((None, PIECE, d), lambda i, s: (s[i],)),
        n * PIECE * d,
        aliases={1 + n: 0},
    )


def after(x, *deps):
    return lax.optimization_barrier((x, *deps))[0]


def solution(mesh):
    n_tp, n_cp = mesh.shape["tp"], mesh.shape["cp"]
    chips = range(n_tp)

    def on_chip(x):
        return lax.ppermute(x, "cp", [(c, n_cp - 1 - c) for c in range(n_cp)])

    def to_chip(x, flip):
        return lax.ppermute(x, "tp", [(i, i ^ flip) for i in chips])

    def to_chip_other(x, flip):
        pairs = [(i * n_cp + c, (i ^ flip) * n_cp + (1 - c)) for i in chips for c in range(n_cp)]
        return lax.ppermute(x, ("tp", "cp"), pairs)

    def to_both(f, x):
        return [f(x, 1), f(x, 2)]

    def spread(m, r):
        return to_both(to_chip, m) + to_both(to_chip_other, r)

    def swap_heads(x):
        return [
            f(x[0, p, 2 * GROUP * i : 2 * GROUP * (i + 1)], 1 + i)
            for p, f in enumerate((to_chip, to_chip_other))
            for i in range(2)
        ]

    def with_partner(ws):
        return [x for w in ws for x in (w, on_chip(w))]

    def relay(w_in, u, dep):
        ws = [after(w_in[a, u], dep) for a in (1, 2)]
        return with_partner(ws), to_chip(ws[u], 2 - u)

    def local_program(hidden, grad, w_query, w_key, w_value, w_out):
        t, c = lax.axis_index("tp"), lax.axis_index("cp")
        chain = [jnp.stack([t, c]).astype(jnp.int32)]

        def step(f, *args, **kw):
            out = f(chain[0], *args, **kw)
            chain[0] = after(chain[0], jax.tree.leaves(out)[0])
            return out

        cos, sin = rope_angles(ROWS)
        tables = lanes([cos, cos]), lanes([-sin, sin])
        tables_t = cos.T, sin.T
        wq, wo = w_query.transpose(1, 0, 2), w_out
        kv_w = (w_key, w_value)
        own, ext, nx, ny = 2 * t, 2 * (3 - t), 2 * (t ^ 1), 2 * (t ^ 2)
        theirs = jnp.stack([own + 1 - c, ext + 1 - c]).astype(jnp.int32)
        unit = lambda u: (2 * c + u).astype(jnp.int32)[None]

        wq_in, wo_in = {}, {}
        sent = pick(unit(0), wq, UNIT)
        for a in (1, 2):
            wq_in[a, 0] = to_chip(sent, a)
        sent = pick(after(theirs, sent), hidden, 1)
        h_recv = on_chip(sent)
        sent = pick(after(unit(0), sent), wo, UNIT)
        for a in (1, 2):
            wo_in[a, 0] = to_chip(sent, a)
        sent = pick(after(theirs, sent), grad, 1)
        g_recv = on_chip(sent)

        k, v, q_0 = step(proj, "q", hidden, h_recv, [wq], tables, kv=kv_w)
        sent_q = pick(after(unit(1), q_0), wq, UNIT)
        sent_o = pick(after(unit(1), sent_q), wo, UNIT)
        for w_in, sent in ((wq_in, sent_q), (wo_in, sent_o)):
            for a in (1, 2):
                w_in[a, 1] = to_chip(sent, a)
        chain[0] = after(chain[0], sent_o)
        (do_0,) = step(proj, "do", grad, g_recv, [wo])
        wq_n0, wq_d0 = relay(wq_in, 0, do_0)
        o_0, dq_0, dk_0, dv_0, t_0 = step(attention, "fused", q_0, k, v, do_0, tables_t, turned=OWN)
        dwo = step(dw_local, 0, t_0, grad, g_recv)

        wo_n0, wo_d0 = relay(wo_in, 0, dwo)
        (q_n0,) = step(proj, "q", hidden, h_recv, wq_n0, tables)
        wq_n1, wq_d1 = relay(wq_in, 1, q_n0)
        (do_n0,) = step(proj, "do", grad, g_recv, wo_n0)
        (q_n1,) = step(proj, "q", hidden, h_recv, wq_n1, tables)
        wo_n1, wo_d1 = relay(wo_in, 1, q_n1)
        o_n0, dq_n0, dk_n0, dv_n0, t_n0 = step(attention, "fused", q_n0, k, v, do_n0, tables_t, turned=0)
        (do_n1,) = step(proj, "do", grad, g_recv, wo_n1)
        wq_d = with_partner([after(w, do_n1) for w in (wq_d0, wq_d1)])
        o_n1, dq_n1, dk_n1, dv_n1, t_n1 = step(attention, "fused", q_n1, k, v, do_n1, tables_t, turned=1, prior=[t_n0])
        t_nb = swap_heads(t_n1)

        (q_d,) = step(proj, "q", hidden, h_recv, wq_d, tables)
        wo_d = with_partner([after(w, q_d) for w in (wo_d0, wo_d1)])
        wo_all = [wo, *wo_n0, *wo_n1, *wo_d]
        wq_all = [wq, *wq_n0, *wq_n1, *wq_d]
        o_d, ot_d, lse_d = step(attention, "fwd", q_d, k, v, nl=1)
        out_big, out_r, out_m = step(combine, "out", 0, [o_0, o_n0, o_n1, o_d], [0] * 4, wo_all)
        out_m = to_both(to_chip, out_m)
        (do_d,) = step(proj, "do", grad, g_recv, wo_d)
        dq_d, dk_d, dv_d = step(attention, "bwd", q_d, k, v, do_d, tables_t, saved=[ot_d, lse_d], nl=1)

        def finish_kv(l, *last):
            dk, dv = [
                x[l] + y[l] + z[l] + w[0]
                for x, y, z, w in zip((dk_0, dv_0), (dk_n0, dv_n0), (dk_n1, dv_n1), last, strict=True)
            ]
            dk = dk * tables[0] - jnp.roll(dk, HALF, axis=1) * tables[1]
            x = jnp.stack([dk, dv]).astype(BF16).reshape(2, 2, PIECE, E).transpose(1, 0, 2, 3)
            x = jnp.where(c == 0, x, x[::-1])
            return x[None], x.transpose(0, 1, 3, 2)

        dkv_0, dkv_t = finish_kv(0, dk_d, dv_d)
        kv_nb = spread(dkv_t[0], dkv_t[1])
        out_r = after(out_r, dkv_t)
        out_r = to_both(to_chip_other, out_r) + [on_chip(out_r)]
        dh_big, dh_r, dh_m = step(combine, "dh", 0, [dq_0, dq_n0, dq_n1, dq_d, dkv_0], [0] * 5, wq_all, kv=kv_w)
        dh_in = spread(dh_m, dh_r) + [on_chip(dh_r)]

        o_e, dq_e, dk_e, dv_e = step(attention, "fused", q_d, k, v, do_d, tables_t, l0=1, nl=1)
        dkv_1, dkv_u = finish_kv(1, dk_e, dv_e)

        (wo_part,) = step(dw_rest, 1, t_nb, grad, dwo)
        wo_part = on_chip(wo_part)
        dw_args = t_0, dkv_t, dkv_u, t_nb, kv_nb, hidden, h_recv
        (wq_part,) = step(dw_in, 1, *dw_args)
        wq_part = on_chip(wq_part)
        dwo_big, dwo_mine = step(dw_rest, 0, t_nb, grad, dwo, wo_part)
        dwo_theirs = on_chip(dwo_mine)
        dwq_big, dwq_mine, dkv_mine = step(dw_in, 0, *dw_args, wq_part)
        dwq_theirs = on_chip(dwq_mine)
        dkv_theirs = on_chip(dkv_mine)

        acts = [dq_0, dq_n0, dq_n1, dq_e, dkv_1]
        side = out_big, out_m + out_r, [*NEAR, (0, 1)], dwo_big, dwo_theirs
        dh_big, dh_er, out_big, d_w_out = step(
            combine, "dh", 1, acts, [1, 1, 1, 0, 0], wq_all, kv=kv_w, big=dh_big, side=side
        )
        dh_er = on_chip(dh_er)
        early = dh_in[:2] + dh_in[4:]
        side = dh_big, early, [*NEAR[:2], (0, 1)], dwq_big, dwq_theirs
        out_big, out_er, dh_big, dwq = step(
            combine, "out", 1, [o_0, o_n0, o_n1, o_e], [1, 1, 1, 0], wo_all, big=out_big, side=side
        )
        out_er = on_chip(out_er)
        late = jnp.stack([nx + 1 - c, ny + 1 - c, ext + 1 - c]).astype(jnp.int32)
        d_hidden = place(after(late, out_er), dh_big, [*dh_in[2:4], dh_er])
        attn_out = place(late[2:], out_big, [out_er])
        d_w_key = jnp.where(c == 0, dkv_mine, dkv_theirs)
        d_w_value = jnp.where(c == 0, dkv_theirs, dkv_mine)
        return attn_out, d_hidden, dwq.transpose(1, 0, 2), d_w_key, d_w_value, d_w_out

    row = P(None, "cp", None)
    wq_spec, wo_spec = P(None, "tp", None), P("tp", None, None)
    return jax.shard_map(
        local_program,
        mesh=mesh,
        in_specs=(row, row, wq_spec, P(), P(), wo_spec),
        out_specs=(row, row, wq_spec, P(), P(), wo_spec),
        check_vma=False,
    )
```

```python
import functools

import jax
import jax.numpy as jnp
import numpy as np
from jax import lax
from jax.experimental import pallas as pl
from jax.experimental.pallas import tpu as pltpu
from jax.sharding import PartitionSpec as P


F32 = jnp.float32
BF16 = jnp.bfloat16
ROPE_BASE = 10000.0
VMEM_LIMIT = 67043328
PIECE = 512
SUB = 256
E = 128
HALF = E // 2
ROWS = 2 * PIECE
N_SUB = ROWS // SUB
N_TILE = N_SUB * (N_SUB + 1) // 2
GROUP = 6
UNIT = 3
WIDE = GROUP * E
COLS = 512
DW_COLS = 1024
SCALE = E**-0.5
OWN = "own"
ALL = slice(None)
HBM = pl.BlockSpec(memory_space=pl.ANY)


def rope_tables(n_pos):
    inv_freq = 1.0 / np.power(np.float32(ROPE_BASE), np.arange(HALF, dtype=np.float32) * np.float32(2.0 / E))
    angles = np.arange(n_pos, dtype=np.float32)[:, None] * inv_freq.astype(np.float32)[None, :]
    return np.cos(angles), np.sin(angles)


def dot_nn(a, b):
    return jnp.dot(a, b, preferred_element_type=F32)


def dot_nt(a, b):
    return lax.dot_general(a, b, (((1,), (1,)), ((), ())), preferred_element_type=F32)


def lanes(parts):
    return jnp.concatenate(parts, axis=1)


def stack(parts):
    return jnp.concatenate(parts, axis=0)


def rows(p):
    return slice(PIECE * p, PIECE * (p + 1))


def heads(e):
    return slice(E * e, E * (e + 1))


def spec(block, index=None, once=False):
    rank = len(block)

    def full(*a):
        i = tuple(index(*a)) if index else ()
        return i + (0,) * (rank - len(i))

    mode = {"pipeline_mode": pl.Buffered(1)} if once or not index else {}
    return pl.BlockSpec(block, full, **mode)


def struct(dtype, *shape):
    return jax.ShapeDtypeStruct(shape, dtype)


def call(body, grid, scal, ins, in_specs, outs, out_specs, flops, scratch=(), aliases=None):
    nbytes = sum(x.size * x.dtype.itemsize for x in jax.tree.leaves([ins, outs]))
    return pl.pallas_call(
        body,
        grid_spec=pltpu.PrefetchScalarGridSpec(
            num_scalar_prefetch=1, grid=grid, in_specs=in_specs, out_specs=out_specs, scratch_shapes=scratch
        ),
        out_shape=outs,
        input_output_aliases=aliases or {},
        cost_estimate=pl.CostEstimate(flops=int(flops), bytes_accessed=int(nbytes), transcendentals=0),
        compiler_params=pltpu.CompilerParams(vmem_limit_bytes=VMEM_LIMIT),
    )(scal, *ins)


def seq_of(l, s):
    return 2 * jnp.where(l == 0, s[0], 3 - s[0]) + s[1]


def in_flight(n, steps, chunks, buf, sem, first=0):
    def load(i):
        return pltpu.make_async_copy(chunks[i][0], buf.at[i % 2], sem.at[0, i % 2])

    def save(i):
        return pltpu.make_async_copy(buf.at[i % 2], chunks[i][1], sem.at[1, i % 2])

    def at(i, *work):
        @pl.when(n == i)
        def _():
            for f, copy in work:
                getattr(copy, f)()

    count = len(chunks)
    for i in range(count):
        done = [("wait", save(i - 2))] if i > 1 else []
        at(first + i, *done, ("start", load(i)))
        at(first + i + 1, ("wait", load(i)), ("start", save(i)))
    return lambda: at(steps - 1, *(("wait", save(i)) for i in range(max(count - 2, 0), count)))


def proj_body(kind, n_w, n_kv, steps, nl, moves, s_ref, x_ref, r_ref, *refs):
    queries = kind == "q"
    if queries:
        cos_ref, sin_ref, *refs = refs
    w_refs, kv_refs, refs = refs[:n_w], refs[n_w : n_w + n_kv], refs[n_w + n_kv :]
    l, n = pl.program_id(0), pl.program_id(1)
    c = s_ref[1]
    finish = []
    if moves:
        side, out, *moved, a_buf, w_buf, kv_buf, a_sem, w_sem, kv_sem, buf_0, sem_0, buf_1, sem_1 = refs
        outs = [out]
        for src, dst, buf, sem in zip((w_refs[0], side), moved, (buf_0, buf_1), (sem_0, sem_1), strict=True):
            chunks = [(src.at[UNIT * (2 * c + 1) + i], dst.at[i]) for i in range(UNIT)]
            finish.append(in_flight(steps * l + n, nl * steps, chunks, buf, sem))
    else:
        *outs, a_buf, w_buf, kv_buf, a_sem, w_sem, kv_sem = refs
    per = n_w // steps if n_w > 1 else 1
    size = GROUP // per

    def row_copies(i):
        parts = (x_ref, seq_of(i, s_ref)), (r_ref, i)
        return [pltpu.make_async_copy(x.at[at], a_buf.at[i, p], a_sem.at[i, p]) for p, (x, at) in enumerate(parts)]

    def weight_copies(j):
        copies = []
        for m in range(per):
            src = w_refs[per * j + m] if n_w > 1 else w_refs[0].at[pl.ds(GROUP * jnp.bitwise_xor(j, c), GROUP)]
            copies.append(pltpu.make_async_copy(src, w_buf.at[pl.ds(GROUP * j + size * m, size)], w_sem.at[j, m]))
        return copies

    def kv_copies():
        return [pltpu.make_async_copy(r, kv_buf.at[i], kv_sem.at[i]) for i, r in enumerate(kv_refs)]

    def at_step(i, j, f, copies):
        @pl.when(jnp.logical_and(l == i, n == j))
        def _():
            for copy in copies():
                getattr(copy, f)()

    def product(ws):
        return dot_nn(stack([a_buf[l, p] for p in range(2)]), lanes(ws))

    def rotated(x, p):
        at = pl.ds(pl.multiple_of(PIECE * jnp.bitwise_xor(p, c), PIECE), PIECE)
        return x * cos_ref[at, :] + pltpu.roll(x, HALF, 1) * sin_ref[at, :]

    now = lambda: row_copies(0) + weight_copies(0)
    later = lambda: sum([*map(weight_copies, range(1, steps)), kv_copies(), *map(row_copies, range(1, nl))], [])
    at_step(0, 0, "start", now)
    at_step(0, 0, "wait", now)
    at_step(0, 0, "start", later)
    for i in range(1, nl):
        at_step(i, 0, "wait", functools.partial(row_copies, i))
    for j in range(1, steps):
        at_step(0, j, "wait", functools.partial(weight_copies, j))

    @pl.when(n < steps)
    def _():
        if queries:
            x = product([w_buf[GROUP * n + e] for e in range(GROUP)])
        else:
            w = w_buf[pl.ds(GROUP * n, GROUP)]
            x = dot_nt(stack([a_buf[l, p] for p in range(2)]), w.reshape(WIDE, w.shape[2]))
        for p in range(2):
            for e in range(GROUP):
                part = x[rows(p), heads(e)]
                outs[0][p, e] = (rotated(part, p) * SCALE if queries else part).astype(BF16)

    if n_kv:
        at_step(0, steps, "wait", kv_copies)

        @pl.when(n == steps)
        def _():
            x = product([kv_buf[i] for i in range(n_kv)])
            for p in range(2):
                outs[1][p] = rotated(x[rows(p), :E], p).astype(BF16)
                outs[2][p] = x[rows(p), E:].astype(BF16)

    for f in finish:
        f()


def proj(scal, kind, x, x_recv, weights, tables=(), kv=(), nl=2, side=()):
    d = x.shape[-1]
    steps = 2 if len(weights) == 1 else len(weights) // 2
    shape = (d, E) if kind == "q" else (E, d)
    dma = pltpu.SemaphoreType.DMA
    last = steps - 1
    moved = [*weights, *side] if side else []
    return call(
        functools.partial(proj_body, kind, len(weights), len(kv), steps, nl, len(side)),
        (nl, steps + len(kv) // 2),
        scal,
        [x, x_recv, *tables, *weights, *kv, *side],
        [HBM] * 2 + [spec((ROWS, E))] * len(tables) + [HBM] * (len(weights) + len(kv) + len(side)),
        [struct(BF16, nl, 2, steps * GROUP, PIECE, E)]
        + [struct(BF16, nl, 2, PIECE, E)] * len(kv)
        + [struct(BF16, UNIT, *w.shape[1:]) for w in moved],
        [spec((None, 2, GROUP, PIECE, E), lambda l, n, s: (l, 0, jnp.minimum(n, last)))]
        + [spec((None, 2, PIECE, E), lambda l, n, s: (l,))] * len(kv)
        + [HBM] * len(moved),
        2 * nl * ROWS * d * steps * WIDE,
        scratch=[
            pltpu.VMEM((nl, 2, PIECE, d), BF16),
            pltpu.VMEM((steps * GROUP, *shape), BF16),
            pltpu.VMEM((len(kv) or 1, d if kv else GROUP, E), BF16),
            dma((nl, 2)),
            dma((steps, 2)),
            dma((2,)),
            *(x for w in moved for x in (pltpu.VMEM((2, *w.shape[1:]), BF16), dma((2, 2)))),
        ],
    )


TRIO = 3


def over_keys(f, x):
    return f(x, axis=0, keepdims=True)


PART = 32


def weave(*lists):
    order = sorted((i / len(fs), j, f) for j, fs in enumerate(lists) for i, f in enumerate(fs))
    for _, _, f in order:
        f()


def attn_body(mode, turned, joined, s_ref, *refs):
    it = iter(refs)
    fwd, bwd = mode != "bwd", mode != "fwd"
    q_ref, k_ref, v_ref = next(it), next(it), next(it)
    if bwd:
        do_ref, cos_ref, sin_ref = next(it), next(it), next(it)
    if not fwd:
        ot_ref, lse_ref = next(it), next(it)
    if joined:
        next(it)
    if fwd:
        o_ref = next(it)
    if not bwd:
        ot_ref, lse_ref = next(it), next(it)
    if bwd:
        dq_ref, dk_ref, dv_ref = next(it), next(it), next(it)
    if turned:
        t_ref = next(it)
    keys, vals, keys_t, vals_t, s_bufs, p_buf, ds_buf = it
    slot = [jnp.bitwise_xor(p, s_ref[1]) for p in range(2)]

    @pl.when(pl.program_id(1) == 0)
    def _():
        for p in range(2):
            kb, vb = k_ref[slot[p]], v_ref[slot[p]]
            keys[rows(p), :] = kb
            vals[rows(p), :] = vb
            keys_t[:, rows(p)] = kb.astype(F32).T.astype(BF16)
            vals_t[:, rows(p)] = vb.astype(F32).T.astype(BF16)
        if bwd:
            dk_ref[...] = jnp.zeros_like(dk_ref)
            dv_ref[...] = jnp.zeros_like(dv_ref)

    iota = functools.partial(lax.broadcasted_iota, jnp.int32, (SUB, SUB))
    causal = iota(0) <= iota(1)
    subs = range(N_SUB)
    tiles = [(i, j) for i in subs for j in range(i + 1)]
    tile = lambda j: slice(SUB * j, SUB * (j + 1))
    per = PIECE // SUB
    base = lambda i, j: tile(i * (i + 1) // 2 + j)
    here = lambda i, h: (slot[i // per], h)
    q = [[q_ref[(*here(i, h), tile(i % per))] for i in subs] for h in range(TRIO)]
    d_o = [[do_ref[(*here(i, h), tile(i % per))] for i in subs] for h in range(TRIO)] if bwd else None

    def phases(h):
        top, inv, total, out_t, delta = {}, {}, {}, {}, {}
        s_buf = s_bufs.at[h]

        def score(i, j):
            s = dot_nt(keys[tile(j), :], q[h][i])
            return jnp.where(causal, s, -jnp.inf) if j == i else s

        def add(sums, i, first, x, f):
            sums[i] = x if first else f(sums[i], x)

        def fold(x, f):
            return f(x.reshape(PART // 8, 8, SUB), axis=0)

        def parts(i, j):
            start = base(i, j).start
            return [(slice(PART * r, PART * (r + 1)), slice(start + PART * r, start + PART * (r + 1))) for r in range(SUB // PART)]

        def scores(i, j):
            s = score(i, j)
            for r, at in parts(i, j):
                s_buf[at, :] = s[r]
                add(top, i, j == 0 and r.start == 0, fold(s[r], jnp.max), jnp.maximum)
            if j == i:
                top[i] = over_keys(jnp.max, top[i])

        def weights(i, j):
            for r, at in parts(i, j):
                p = jnp.exp(s_buf[at, :] - top[i])
                if bwd:
                    s_buf[at, :] = p
                add(total, i, j == 0 and r.start == 0, fold(p, jnp.sum), jnp.add)
                p_buf[h, SUB * j + r.start : SUB * j + r.stop, tile(i)] = p.astype(BF16)
            if j == i:
                width = SUB * (i + 1)
                total[i] = over_keys(jnp.sum, total[i])
                inv[i] = 1.0 / total[i]
                o_t = dot_nn(vals_t[:, :width], p_buf[h, :width, tile(i)]) * inv[i]
                out_t[i] = o_t.astype(BF16)
                o_ref[(*here(i, h), tile(i % per))] = o_t.T.astype(BF16)
                if turned:
                    t_ref[(*here(i, h), 0, ALL, tile(i % per))] = out_t[i]
                if not bwd:
                    ot_ref[(*here(i, h), ALL, tile(i % per))] = out_t[i]
                    lse_ref[h, :, tile(i)] = top[i] + jnp.log(total[i])

        def score_grads(i, j):
            if j == 0:
                o_t = out_t[i] if fwd else ot_ref[(*here(i, h), ALL, tile(i % per))]
                delta[i] = over_keys(jnp.sum, o_t.astype(F32) * d_o[h][i].astype(F32).T)
            s = None if fwd else score(i, j)
            dp = dot_nt(vals[tile(j), :], d_o[h][i])
            for r, at in parts(i, j):
                p = s_buf[at, :] * inv[i] if fwd else jnp.exp(s[r] - lse_ref[h, :, tile(i)])
                to = slice(SUB * j + r.start, SUB * j + r.stop)
                p_buf[h, to, tile(i)] = p.astype(BF16)
                ds_buf[h, to, tile(i)] = (p * (dp[r] - delta[i])).astype(BF16)

        def query_grads(i):
            width = SUB * (i + 1)
            dq = dot_nn(keys_t[:, :width], ds_buf[h, :width, tile(i)]) * SCALE
            low, high, cos, sin = dq[:HALF], dq[HALF:], cos_ref[:, tile(i)], sin_ref[:, tile(i)]
            dq = stack([low * cos + high * sin, high * cos - low * sin])
            dq_ref[(*here(i, h), tile(i % per))] = dq.T.astype(BF16)
            if turned:
                t_ref[(*here(i, h), 1, ALL, tile(i % per))] = dq.astype(BF16)

        def key_grads(j):
            dv_ref[tile(j), :] += dot_nn(p_buf[h, tile(j), SUB * j :], stack(d_o[h][j:]))
            dk_ref[tile(j), :] += dot_nn(ds_buf[h, tile(j), SUB * j :], stack(q[h][j:]))

        each = lambda f, some: [functools.partial(f, *x) for x in some]
        lists = [each(scores, tiles), each(weights, tiles)] if fwd else []
        if bwd:
            alone = [(i,) for i in subs]
            lists += [each(score_grads, tiles), each(query_grads, alone) + each(key_grads, alone)]
        return lists

    work = [phases(h) for h in range(TRIO)]
    n_phases = len(work[0])
    for stage in range(TRIO + n_phases - 1):
        weave(*(work[h][stage - h] for h in range(TRIO) if 0 <= stage - h < n_phases))


def attention(scal, mode, q, k, v, d_o=None, tables=(), saved=(), l0=0, nl=2, turned=None, prior=()):
    n_heads = q.shape[2]
    fwd, bwd = mode != "bwd", mode != "fwd"
    at_in, at_out = lambda l, h, s: (l + l0, 0, h), lambda l, h, s: (l, 0, h)
    block = (None, 2, TRIO, PIECE, E)
    act_in, act = spec(block, at_in), spec(block, at_out)
    flat = spec((None, 2, TRIO, E, PIECE), at_out)
    kv_spec = spec((None, 2, PIECE, E), lambda l, h, s: (l + l0,))
    stat = spec((None, TRIO, 1, ROWS), lambda l, h, s: (l, h))
    acc = spec((None, ROWS, E), lambda l, h, s: (l,))
    ins, specs, outs, out_specs = [q, k, v], [act_in, kv_spec, kv_spec], [], []
    act_shape = struct(BF16, nl, 2, n_heads, PIECE, E)
    if bwd:
        ins += [d_o, *tables]
        specs += [act_in] + [spec((HALF, ROWS))] * 2
    if not fwd:
        ins += saved
        specs += [flat, stat]
    if fwd:
        outs.append(act_shape)
        out_specs.append(act)
    if not bwd:
        outs += [struct(BF16, nl, 2, n_heads, E, PIECE), struct(F32, nl, n_heads, 1, ROWS)]
        out_specs += [flat, stat]
    if bwd:
        outs += [act_shape] + [struct(F32, nl, ROWS, E)] * 2
        out_specs += [act, acc, acc]
    if turned is not None:
        per = GROUP // TRIO
        shift = 0 if turned == OWN else per
        outs.append(struct(BF16, nl, 2, n_heads * (2 if shift else 1), 2, E, PIECE))
        place_head = lambda l, h, s: (l, 0, h + (per * (h // per + turned) if shift else 0))
        out_specs.append(spec((None, 2, TRIO, 2, E, PIECE), place_head))
    aliases = {1 + len(ins): len(outs) - 1} if prior else {}
    ins += prior
    specs += [HBM] * len(prior)
    products = 2 * fwd + 4 * bwd + (not fwd)
    square = TRIO, ROWS, ROWS
    return call(
        functools.partial(attn_body, mode, turned is not None, len(prior)),
        (nl, n_heads // TRIO),
        scal,
        ins,
        specs,
        outs,
        out_specs,
        nl * n_heads * products * 4 * E * SUB * SUB * N_TILE,
        scratch=[pltpu.VMEM((ROWS, E), BF16)] * 2
        + [pltpu.VMEM((E, ROWS), BF16)] * 2
        + [pltpu.VMEM((TRIO, N_TILE * SUB if fwd else SUB, SUB), F32)]
        + [pltpu.VMEM(square, BF16)] * 2,
        aliases=aliases,
    )


def seq_near(s, flip, other):
    return 2 * jnp.bitwise_xor(s[0], flip) + jnp.bitwise_xor(s[1], other)


def combine_body(kind, n_act, n_w, near, fresh, steps, s_ref, *refs):
    acts, ws, refs = refs[:n_act], refs[n_act : n_act + n_w], refs[n_act + n_w :]
    c, n = s_ref[1], pl.program_id(0)
    if kind == "dh":
        kv_refs, refs = refs[:2], refs[2:]
    if not fresh:
        refs = refs[1:]
    finish = []
    if near:
        pieces, theirs, refs = refs[2 : 2 + len(near)], refs[2 + len(near)], refs[len(near) + 3 :]
        *refs, rows_out, grad_out, row_buf, grad_buf, row_sem, grad_sem = refs
        row_chunks = [
            (r.at[cut], rows_out.at[seq_near(s_ref, *at), cut])
            for r, at in zip(pieces, near, strict=True)
            for cut in (pl.ds(SUB * i, SUB) for i in range(PIECE // SUB))
        ]
        grad_chunks = [(theirs.at[i], grad_out.at[GROUP * (1 - c) + i]) for i in range(GROUP)]
        finish.append(in_flight(n, steps, row_chunks, row_buf, row_sem))
        finish.append(in_flight(n, steps, grad_chunks, grad_buf, grad_sem, first=steps - GROUP - 1))
    a = lanes([stack([r[0, h], r[1, h]]) for r in acts for h in range(r.shape[1])])
    held = [ws[0][pl.ds(GROUP * i, GROUP)] for i in (c, 1 - c)] + [w[...] for w in ws[1:]]
    if kind == "out":
        x = dot_nn(a, stack([w.reshape(w.shape[0] * E, w.shape[2]) for w in held]))
    else:
        x = dot_nt(a, lanes([w[h] for w in held for h in range(w.shape[0])] + [r[...] for r in kv_refs]))
    x = x.astype(BF16)
    refs[0][...] = x[rows(0)]
    refs[1][...] = x[rows(1)]
    if fresh:
        refs[2][...] = x[rows(0)]
    for f in finish:
        f()


def combine(scal, kind, l, acts, weights, kv=(), big=None, side=None):
    d = weights[0].shape[2 if kind == "out" else 1]
    steps = d // COLS
    in_specs = [
        spec((None, 2, a.shape[2], PIECE, E), lambda n, s, i=min(l, a.shape[0] - 1): (i,), once=True) for a in acts
    ]
    if kind == "out":
        in_specs += [spec((w.shape[0], E, COLS), lambda n, s: (0, 0, n)) for w in weights]
    else:
        in_specs += [spec((w.shape[0], COLS, E), lambda n, s: (0, n)) for w in weights]
        in_specs += [spec((COLS, E), lambda n, s: (n,))] * 2
    piece = spec((PIECE, COLS), lambda n, s: (0, n))
    fresh = big is None
    ins, aliases, scratch, near = [*acts, *weights, *kv], {}, [], ()
    outs = [struct(BF16, 8, PIECE, d)] + [struct(BF16, PIECE, d)] * (1 + fresh)
    out_specs = [spec((None, PIECE, COLS), lambda n, s: (seq_of(l, s), 0, n))] + [piece] * (1 + fresh)
    moved = [] if fresh else [big]
    if side:
        whole, pieces, near, grad, theirs = side
        moved += [whole, grad, *pieces, theirs]
        outs += [struct(x.dtype, *x.shape) for x in (whole, grad)]
        out_specs += [HBM] * 2
        dma = pltpu.SemaphoreType.DMA
        scratch = [
            pltpu.VMEM((2, SUB, d), BF16),
            pltpu.VMEM((2, *theirs.shape[1:]), F32),
            dma((2, 2)),
            dma((2, 2)),
        ]
    for i, o in zip(range(3 if side else len(moved)), (0, 2, 3), strict=False):
        aliases[1 + len(ins) + i] = o
    return call(
        functools.partial(combine_body, kind, len(acts), len(weights), near, fresh, steps),
        (steps,),
        scal,
        ins + moved,
        in_specs + [HBM] * len(moved),
        outs,
        out_specs,
        2 * ROWS * sum(a.shape[2] for a in acts) * E * d,
        scratch=scratch,
        aliases=aliases,
    )


def dw_local_body(s_ref, t_ref, *refs):
    xs, o_ref = refs[:4], refs[4]
    a = lanes([stack([t_ref[l, p, h] for h in range(t_ref.shape[2])]) for l in range(2) for p in range(2)])
    o_ref[...] = dot_nn(a, stack([x[...] for x in xs])).reshape(o_ref.shape)


def dw_local(scal, which, turned, x, x_recv):
    d = x.shape[-1]
    block = (None, PIECE, DW_COLS)
    mine = [spec(block, lambda n, s, l=l: (seq_of(l, s), 0, n)) for l in range(2)]
    recv = [spec(block, lambda n, s, l=l: (l, 0, n)) for l in range(2)]
    n_heads = turned.shape[2]
    return call(
        dw_local_body,
        (d // DW_COLS,),
        scal,
        [turned, x, x_recv, x, x_recv],
        [spec((2, 2, n_heads, None, E, PIECE), lambda n, s: (0, 0, 0, which)), mine[0], recv[0], mine[1], recv[1]],
        struct(F32, n_heads, E, d),
        spec((n_heads, E, DW_COLS), lambda n, s: (0, 0, n)),
        4 * n_heads * E * ROWS * d,
    )


def dw_rest_body(last, s_ref, *refs):
    ts, xs, refs = refs[:8], refs[8:12], refs[12:]
    a = lanes([stack([t[h] for t in ts[2 * g : 2 * g + 2] for h in range(UNIT)]) for g in range(4)])
    acc = dot_nn(a, stack([x[...] for x in xs])).reshape(GROUP, E, DW_COLS) + refs[0][...]
    if last:
        acc = acc + refs[1][...]
    for o in refs[-2:] if last else refs[-1:]:
        o[...] = acc


NEAR = tuple((flip, other) for other in range(2) for flip in (1, 2))


def near_specs(half, which):
    specs = []
    for _, other in NEAR:
        i = half ^ other
        specs += [spec((UNIT, None, E, PIECE), lambda n, s, j=j: (j, which)) for j in (i, 2 + i)]
    rows_at = [spec((None, PIECE, DW_COLS), lambda n, s, at=at: (seq_near(s, *at), 0, n)) for at in NEAR]
    return specs, rows_at


def dw_rest(scal, half, turned, x, local, recv=None):
    d = x.shape[-1]
    block, at_n = (GROUP, E, DW_COLS), lambda n, s: (0, 0, n)
    specs, rows_at = near_specs(half, 0)
    specs += rows_at + [spec(block, lambda n, s: (half, 0, n))]
    ins = [*(t for t in turned for _ in range(2)), x, x, x, x, local]
    outs, out_specs = [struct(F32, GROUP, E, d)], [spec(block, at_n)]
    last = recv is not None
    if last:
        ins.append(recv)
        specs.append(spec(block, at_n))
        outs.insert(0, struct(F32, 2 * GROUP, E, d))
        out_specs.insert(0, spec(block, lambda n, s: (s[1], 0, n)))
    return call(
        functools.partial(dw_rest_body, last),
        (d // DW_COLS,),
        scal,
        ins,
        specs,
        outs,
        out_specs,
        4 * GROUP * E * ROWS * d,
    )


def dw_in_body(last, s_ref, t_ref, u0_ref, u1_ref, *refs):
    ts, kvs, xs, refs = refs[:8], refs[8:12], refs[12:20], refs[20:]
    groups = [
        stack([t_ref[l, p, h] for h in range(GROUP)] + [u[p]]) for l, u in enumerate((u0_ref, u1_ref)) for p in range(2)
    ]
    groups += [
        stack([t[h] for t in ts[2 * g : 2 * g + 2] for h in range(UNIT)] + [kvs[g][...]]) for g in range(len(kvs))
    ]
    acc = dot_nn(lanes(groups), stack([x[...] for x in xs])).reshape(GROUP + 1, E, DW_COLS)
    if not last:
        refs[0][...] = acc
        return
    acc = acc + refs[0][...]
    for h in range(GROUP):
        refs[1][h] = refs[2][h] = acc[h].T
    refs[3][...] = acc[GROUP].T


def dw_in(scal, half, turned_0, kv_0, kv_1, turned, kv, x, x_recv, recv=None):
    d = x.shape[-1]
    kv_half = lambda s: jnp.bitwise_xor(half, s[1])
    near, rows_at = near_specs(half, 1)
    local = [spec((2, 2, GROUP, None, E, PIECE), lambda n, s: (0, 0, half, 1))]
    local += [spec((2, None, E, PIECE), lambda n, s: (0, kv_half(s)))] * 2
    block = (None, PIECE, DW_COLS)
    for l in range(2):
        rows_at.insert(2 * l, spec(block, lambda n, s, l=l: (seq_of(l, s), 0, n)))
        rows_at.insert(2 * l + 1, spec(block, lambda n, s, l=l: (l, 0, n)))
    near += [spec((None, E, PIECE), lambda n, s: (kv_half(s),))] * len(kv)
    ins = [turned_0, kv_0, kv_1, *(t for t in turned for _ in range(2)), *kv, x, x_recv, x, x_recv, x, x, x, x]
    specs = local + near + rows_at
    part = spec((GROUP + 1, E, DW_COLS), lambda n, s: (0, 0, n))
    outs, out_specs = [struct(F32, GROUP + 1, E, d)], [part]
    last = recv is not None
    if last:
        ins.append(recv)
        specs.append(part)
        block = (GROUP, DW_COLS, E)
        outs = [struct(F32, 2 * GROUP, d, E), struct(F32, GROUP, d, E), struct(F32, d, E)]
        out_specs = [spec(block, lambda n, s: (s[1], n)), spec(block, lambda n, s: (0, n))]
        out_specs.append(spec((DW_COLS, E), lambda n, s: (n,)))
    return call(
        functools.partial(dw_in_body, last),
        (d // DW_COLS,),
        scal,
        ins,
        specs,
        outs,
        out_specs,
        8 * (GROUP + 1) * E * ROWS * d,
    )


def copy_body(s_ref, x_ref, o_ref):
    o_ref[...] = x_ref[...]


def pick(indices, x, block):
    count, rest = indices.shape[0], x.shape[1:]
    return call(
        copy_body,
        (count,),
        indices,
        [x],
        [spec((block, *rest), lambda i, s: (s[i],))],
        struct(x.dtype, count * block, *rest),
        spec((block, *rest), lambda i, s: (i,)),
        x.size,
    )


def place_body(n, s_ref, *refs):
    for j in range(n):

        @pl.when(pl.program_id(0) == j)
        def _():
            refs[-1][...] = refs[j][...]


def place(seqs, big, pieces):
    n, d = len(pieces), big.shape[-1]
    return call(
        functools.partial(place_body, n),
        (n,),
        seqs,
        [*pieces, big],
        [spec((PIECE, d))] * n + [HBM],
        struct(big.dtype, *big.shape),
        spec((None, PIECE, d), lambda i, s: (s[i],)),
        n * PIECE * d,
        aliases={1 + n: 0},
    )


def after(x, *deps):
    return lax.optimization_barrier((x, *deps))[0]


def solution(mesh):
    n_tp, n_cp = mesh.shape["tp"], mesh.shape["cp"]
    chips = range(n_tp)

    def on_chip(x):
        return lax.ppermute(x, "cp", [(c, n_cp - 1 - c) for c in range(n_cp)])

    def to_chip(x, flip):
        return lax.ppermute(x, "tp", [(i, i ^ flip) for i in chips])

    def to_chip_other(x, flip):
        pairs = [(i * n_cp + c, (i ^ flip) * n_cp + (1 - c)) for i in chips for c in range(n_cp)]
        return lax.ppermute(x, ("tp", "cp"), pairs)

    def to_both(f, x):
        return [f(x, 1), f(x, 2)]

    def spread(m, r):
        return to_both(to_chip, m) + to_both(to_chip_other, r)

    def swap_heads(x):
        return [
            f(x[0, p, 2 * GROUP * i : 2 * GROUP * (i + 1)], 1 + i)
            for p, f in enumerate((to_chip, to_chip_other))
            for i in range(2)
        ]

    def with_partner(ws):
        return [x for w in ws for x in (w, on_chip(w))]

    def relay(w_in, u, dep):
        ws = [after(w_in[a, u], dep) for a in (1, 2)]
        return with_partner(ws), to_chip(ws[u], 2 - u)

    def local_program(hidden, grad, w_query, w_key, w_value, w_out):
        t, c = lax.axis_index("tp"), lax.axis_index("cp")
        chain = [jnp.stack([t, c]).astype(jnp.int32)]

        def step(f, *args, **kw):
            out = f(chain[0], *args, **kw)
            chain[0] = after(chain[0], jax.tree.leaves(out)[0])
            return out

        cos, sin = rope_tables(ROWS)
        tables = [jnp.asarray(np.concatenate(x, axis=1)) for x in ((cos, cos), (-sin, sin))]
        tables_t = [jnp.asarray(np.ascontiguousarray(x.T)) for x in (cos, sin)]
        wq, wo = w_query.transpose(1, 0, 2), w_out
        kv_w = (w_key, w_value)
        own, ext, nx, ny = 2 * t, 2 * (3 - t), 2 * (t ^ 1), 2 * (t ^ 2)
        theirs = jnp.stack([own + 1 - c, ext + 1 - c]).astype(jnp.int32)
        unit = (2 * c).astype(jnp.int32)[None]

        wq_in, wo_in = {}, {}
        sent = pick(theirs, hidden, 1)
        h_recv = on_chip(sent)
        sent = pick(after(unit, sent), wq, UNIT)
        for a in (1, 2):
            wq_in[a, 0] = to_chip(sent, a)
        sent = pick(after(unit, sent), wo, UNIT)
        for a in (1, 2):
            wo_in[a, 0] = to_chip(sent, a)
        g_recv = on_chip(pick(after(theirs, sent), grad, 1))

        q_0, k, v = step(proj, "q", hidden, h_recv, [wq], tables, kv=kv_w)
        do_0, wo_sent, wq_sent = step(proj, "do", grad, g_recv, [wo], side=[wq])
        for a in (1, 2):
            wq_in[a, 1] = to_chip(wq_sent, a)
            wo_in[a, 1] = to_chip(wo_sent, a)
        wq_n0, wq_d0 = relay(wq_in, 0, do_0)
        o_0, dq_0, dk_0, dv_0, t_0 = step(attention, "fused", q_0, k, v, do_0, tables_t, turned=OWN)
        dwo = step(dw_local, 0, t_0, grad, g_recv)

        wo_n0, wo_d0 = relay(wo_in, 0, dwo)
        (q_n0,) = step(proj, "q", hidden, h_recv, wq_n0, tables)
        wq_n1, wq_d1 = relay(wq_in, 1, q_n0)
        (do_n0,) = step(proj, "do", grad, g_recv, wo_n0)
        (q_n1,) = step(proj, "q", hidden, h_recv, wq_n1, tables)
        wo_n1, wo_d1 = relay(wo_in, 1, q_n1)
        o_n0, dq_n0, dk_n0, dv_n0, t_n0 = step(attention, "fused", q_n0, k, v, do_n0, tables_t, turned=0)
        (do_n1,) = step(proj, "do", grad, g_recv, wo_n1)
        wq_d = with_partner([after(w, do_n1) for w in (wq_d0, wq_d1)])
        o_n1, dq_n1, dk_n1, dv_n1, t_n1 = step(attention, "fused", q_n1, k, v, do_n1, tables_t, turned=1, prior=[t_n0])
        t_nb = swap_heads(t_n1)

        (q_d,) = step(proj, "q", hidden, h_recv, wq_d, tables)
        wo_d = with_partner([after(w, q_d) for w in (wo_d0, wo_d1)])
        wo_all = [wo, *wo_n0, *wo_n1, *wo_d]
        wq_all = [wq, *wq_n0, *wq_n1, *wq_d]
        o_d, ot_d, lse_d = step(attention, "fwd", q_d, k, v, nl=1)
        out_big, out_r, out_m = step(combine, "out", 0, [o_0, o_n0, o_n1, o_d], wo_all)
        out_m = to_both(to_chip, out_m)
        (do_d,) = step(proj, "do", grad, g_recv, wo_d)
        dq_d, dk_d, dv_d = step(attention, "bwd", q_d, k, v, do_d, tables_t, saved=[ot_d, lse_d], nl=1)

        def finish_kv(l, *last):
            dk, dv = [
                x[l] + y[l] + z[l] + w[0]
                for x, y, z, w in zip((dk_0, dv_0), (dk_n0, dv_n0), (dk_n1, dv_n1), last, strict=True)
            ]
            dk = dk * tables[0] - jnp.roll(dk, HALF, axis=1) * tables[1]
            x = jnp.stack([dk, dv]).astype(BF16).reshape(2, 2, PIECE, E).transpose(1, 0, 2, 3)
            x = jnp.where(c == 0, x, x[::-1])
            return x[None], x.transpose(0, 1, 3, 2)

        dkv_0, dkv_t = finish_kv(0, dk_d, dv_d)
        kv_nb = spread(dkv_t[0], dkv_t[1])
        out_r = after(out_r, dkv_t)
        out_r = to_both(to_chip_other, out_r) + [on_chip(out_r)]
        dh_big, dh_r, dh_m = step(combine, "dh", 0, [dq_0, dq_n0, dq_n1, dq_d, dkv_0], wq_all, kv=kv_w)
        dh_in = spread(dh_m, dh_r) + [on_chip(dh_r)]

        o_e, dq_e, dk_e, dv_e = step(attention, "fused", q_d, k, v, do_d, tables_t, l0=1, nl=1)
        dkv_1, dkv_u = finish_kv(1, dk_e, dv_e)

        (wo_part,) = step(dw_rest, 1, t_nb, grad, dwo)
        wo_part = on_chip(wo_part)
        dw_args = t_0, dkv_t, dkv_u, t_nb, kv_nb, hidden, h_recv
        (wq_part,) = step(dw_in, 1, *dw_args)
        wq_part = on_chip(wq_part)
        dwo_big, dwo_mine = step(dw_rest, 0, t_nb, grad, dwo, wo_part)
        dwo_theirs = on_chip(dwo_mine)
        dwq_big, dwq_mine, dkv_mine = step(dw_in, 0, *dw_args, wq_part)
        dwq_theirs = on_chip(dwq_mine)
        dkv_theirs = on_chip(dkv_mine)

        acts = [dq_0, dq_n0, dq_n1, dq_e, dkv_1]
        side = out_big, out_m + out_r, [*NEAR, (0, 1)], dwo_big, dwo_theirs
        dh_big, dh_er, out_big, d_w_out = step(combine, "dh", 1, acts, wq_all, kv=kv_w, big=dh_big, side=side)
        dh_er = on_chip(dh_er)
        early = dh_in[:2] + dh_in[4:]
        side = dh_big, early, [*NEAR[:2], (0, 1)], dwq_big, dwq_theirs
        out_big, out_er, dh_big, dwq = step(combine, "out", 1, [o_0, o_n0, o_n1, o_e], wo_all, big=out_big, side=side)
        out_er = on_chip(out_er)
        late = jnp.stack([nx + 1 - c, ny + 1 - c, ext + 1 - c]).astype(jnp.int32)
        d_hidden = place(after(late, out_big), dh_big, [*dh_in[2:4], dh_er])
        attn_out = place(after(late[2:], d_hidden), out_big, [out_er])
        d_w_key = jnp.where(c == 0, dkv_mine, dkv_theirs)
        d_w_value = jnp.where(c == 0, dkv_theirs, dkv_mine)
        return attn_out, d_hidden, dwq.transpose(1, 0, 2), d_w_key, d_w_value, d_w_out

    row = P(None, "cp", None)
    wq_spec, wo_spec = P(None, "tp", None), P("tp", None, None)
    return jax.shard_map(
        local_program,
        mesh=mesh,
        in_specs=(row, row, wq_spec, P(), P(), wo_spec),
        out_specs=(row, row, wq_spec, P(), P(), wo_spec),
        check_vma=False,
    )
```

```python
import functools

import jax
import jax.numpy as jnp
import numpy as np
from jax import lax
from jax.experimental import pallas as pl
from jax.experimental.pallas import tpu as pltpu
from jax.sharding import PartitionSpec as P


F32 = jnp.float32
BF16 = jnp.bfloat16
ROPE_BASE = 10000.0
VMEM_LIMIT = 67043328
PIECE = 512
SUB = 256
E = 128
HALF = E // 2
ROWS = 2 * PIECE
N_SUB = ROWS // SUB
N_TILE = N_SUB * (N_SUB + 1) // 2
GROUP = 6
UNIT = 3
WIDE = GROUP * E
COLS = 512
DW_COLS = 1024
SCALE = E**-0.5
OWN = "own"
ALL = slice(None)
HBM = pl.BlockSpec(memory_space=pl.ANY)


def rope_tables(n_pos):
    inv_freq = 1.0 / np.power(np.float32(ROPE_BASE), np.arange(HALF, dtype=np.float32) * np.float32(2.0 / E))
    angles = np.arange(n_pos, dtype=np.float32)[:, None] * inv_freq.astype(np.float32)[None, :]
    return np.cos(angles), np.sin(angles)


def dot_nn(a, b):
    return jnp.dot(a, b, preferred_element_type=F32)


def dot_nt(a, b):
    return lax.dot_general(a, b, (((1,), (1,)), ((), ())), preferred_element_type=F32)


def lanes(parts):
    return jnp.concatenate(parts, axis=1)


def stack(parts):
    return jnp.concatenate(parts, axis=0)


def rows(p):
    return slice(PIECE * p, PIECE * (p + 1))


def heads(e):
    return slice(E * e, E * (e + 1))


def spec(block, index=None, once=False):
    rank = len(block)

    def full(*a):
        i = tuple(index(*a)) if index else ()
        return i + (0,) * (rank - len(i))

    mode = {"pipeline_mode": pl.Buffered(1)} if once or not index else {}
    return pl.BlockSpec(block, full, **mode)


def struct(dtype, *shape):
    return jax.ShapeDtypeStruct(shape, dtype)


def call(body, grid, scal, ins, in_specs, outs, out_specs, flops, scratch=(), aliases=None):
    nbytes = sum(x.size * x.dtype.itemsize for x in jax.tree.leaves([ins, outs]))
    return pl.pallas_call(
        body,
        grid_spec=pltpu.PrefetchScalarGridSpec(
            num_scalar_prefetch=1, grid=grid, in_specs=in_specs, out_specs=out_specs, scratch_shapes=scratch
        ),
        out_shape=outs,
        input_output_aliases=aliases or {},
        cost_estimate=pl.CostEstimate(flops=int(flops), bytes_accessed=int(nbytes), transcendentals=0),
        compiler_params=pltpu.CompilerParams(vmem_limit_bytes=VMEM_LIMIT),
    )(scal, *ins)


def seq_of(l, s):
    return 2 * jnp.where(l == 0, s[0], 3 - s[0]) + s[1]


def in_flight(n, steps, chunks, buf, sem, first=0):
    def load(i):
        return pltpu.make_async_copy(chunks[i][0], buf.at[i % 2], sem.at[0, i % 2])

    def save(i):
        return pltpu.make_async_copy(buf.at[i % 2], chunks[i][1], sem.at[1, i % 2])

    def at(i, *work):
        @pl.when(n == i)
        def _():
            for f, copy in work:
                getattr(copy, f)()

    count = len(chunks)
    for i in range(count):
        done = [("wait", save(i - 2))] if i > 1 else []
        at(first + i, *done, ("start", load(i)))
        at(first + i + 1, ("wait", load(i)), ("start", save(i)))
    return lambda: at(steps - 1, *(("wait", save(i)) for i in range(max(count - 2, 0), count)))


def proj_body(kind, n_w, n_kv, steps, nl, moves, s_ref, x_ref, r_ref, *refs):
    queries = kind == "q"
    if queries:
        cos_ref, sin_ref, *refs = refs
    w_refs, kv_refs, refs = refs[:n_w], refs[n_w : n_w + n_kv], refs[n_w + n_kv :]
    l, n = pl.program_id(0), pl.program_id(1)
    c = s_ref[1]
    finish = []
    if moves:
        side, out, *moved, a_buf, w_buf, kv_buf, a_sem, w_sem, kv_sem, buf_0, sem_0, buf_1, sem_1 = refs
        outs = [out]
        for src, dst, buf, sem in zip((w_refs[0], side), moved, (buf_0, buf_1), (sem_0, sem_1), strict=True):
            chunks = [(src.at[UNIT * (2 * c + 1) + i], dst.at[i]) for i in range(UNIT)]
            finish.append(in_flight(steps * l + n, nl * steps, chunks, buf, sem))
    else:
        *outs, a_buf, w_buf, kv_buf, a_sem, w_sem, kv_sem = refs
    per = n_w // steps if n_w > 1 else 1
    size = GROUP // per

    def row_copies(i):
        parts = (x_ref, seq_of(i, s_ref)), (r_ref, i)
        return [pltpu.make_async_copy(x.at[at], a_buf.at[i, p], a_sem.at[i, p]) for p, (x, at) in enumerate(parts)]

    def weight_copies(j):
        copies = []
        for m in range(per):
            src = w_refs[per * j + m] if n_w > 1 else w_refs[0].at[pl.ds(GROUP * jnp.bitwise_xor(j, c), GROUP)]
            copies.append(pltpu.make_async_copy(src, w_buf.at[pl.ds(GROUP * j + size * m, size)], w_sem.at[j, m]))
        return copies

    def kv_copies():
        return [pltpu.make_async_copy(r, kv_buf.at[i], kv_sem.at[i]) for i, r in enumerate(kv_refs)]

    def at_step(i, j, f, copies):
        @pl.when(jnp.logical_and(l == i, n == j))
        def _():
            for copy in copies():
                getattr(copy, f)()

    def product(ws):
        return dot_nn(stack([a_buf[l, p] for p in range(2)]), lanes(ws))

    def rotated(x, p):
        at = pl.ds(pl.multiple_of(PIECE * jnp.bitwise_xor(p, c), PIECE), PIECE)
        return x * cos_ref[at, :] + pltpu.roll(x, HALF, 1) * sin_ref[at, :]

    now = lambda: row_copies(0) + weight_copies(0)
    later = lambda: sum([*map(weight_copies, range(1, steps)), kv_copies(), *map(row_copies, range(1, nl))], [])
    at_step(0, 0, "start", now)
    at_step(0, 0, "wait", now)
    at_step(0, 0, "start", later)
    for i in range(1, nl):
        at_step(i, 0, "wait", functools.partial(row_copies, i))
    for j in range(1, steps):
        at_step(0, j, "wait", functools.partial(weight_copies, j))

    @pl.when(n < steps)
    def _():
        if queries:
            x = product([w_buf[GROUP * n + e] for e in range(GROUP)])
        else:
            w = w_buf[pl.ds(GROUP * n, GROUP)]
            x = dot_nt(stack([a_buf[l, p] for p in range(2)]), w.reshape(WIDE, w.shape[2]))
        for p in range(2):
            for e in range(GROUP):
                part = x[rows(p), heads(e)]
                outs[0][p, e] = (rotated(part, p) * SCALE if queries else part).astype(BF16)

    if n_kv:
        at_step(0, steps, "wait", kv_copies)

        @pl.when(n == steps)
        def _():
            x = product([kv_buf[i] for i in range(n_kv)])
            for p in range(2):
                outs[1][p] = rotated(x[rows(p), :E], p).astype(BF16)
                outs[2][p] = x[rows(p), E:].astype(BF16)

    for f in finish:
        f()


def proj(scal, kind, x, x_recv, weights, tables=(), kv=(), nl=2, side=()):
    d = x.shape[-1]
    steps = 2 if len(weights) == 1 else len(weights) // 2
    shape = (d, E) if kind == "q" else (E, d)
    dma = pltpu.SemaphoreType.DMA
    last = steps - 1
    moved = [*weights, *side] if side else []
    return call(
        functools.partial(proj_body, kind, len(weights), len(kv), steps, nl, len(side)),
        (nl, steps + len(kv) // 2),
        scal,
        [x, x_recv, *tables, *weights, *kv, *side],
        [HBM] * 2 + [spec((ROWS, E))] * len(tables) + [HBM] * (len(weights) + len(kv) + len(side)),
        [struct(BF16, nl, 2, steps * GROUP, PIECE, E)]
        + [struct(BF16, nl, 2, PIECE, E)] * len(kv)
        + [struct(BF16, UNIT, *w.shape[1:]) for w in moved],
        [spec((None, 2, GROUP, PIECE, E), lambda l, n, s: (l, 0, jnp.minimum(n, last)))]
        + [spec((None, 2, PIECE, E), lambda l, n, s: (l,))] * len(kv)
        + [HBM] * len(moved),
        2 * nl * ROWS * d * steps * WIDE,
        scratch=[
            pltpu.VMEM((nl, 2, PIECE, d), BF16),
            pltpu.VMEM((steps * GROUP, *shape), BF16),
            pltpu.VMEM((len(kv) or 1, d if kv else GROUP, E), BF16),
            dma((nl, 2)),
            dma((steps, 2)),
            dma((2,)),
            *(x for w in moved for x in (pltpu.VMEM((2, *w.shape[1:]), BF16), dma((2, 2)))),
        ],
    )


TRIO = 3


def over_keys(f, x):
    return f(x, axis=0, keepdims=True)


PART = 32


def weave(*lists):
    order = sorted((i / len(fs), j, f) for j, fs in enumerate(lists) for i, f in enumerate(fs))
    for _, _, f in order:
        f()


def attn_body(mode, turned, joined, s_ref, *refs):
    it = iter(refs)
    fwd, bwd = mode != "bwd", mode != "fwd"
    q_ref, k_ref, v_ref = next(it), next(it), next(it)
    if bwd:
        do_ref, cos_ref, sin_ref = next(it), next(it), next(it)
    if not fwd:
        ot_ref, lse_ref = next(it), next(it)
    if joined:
        next(it)
    if fwd:
        o_ref = next(it)
    if not bwd:
        ot_ref, lse_ref = next(it), next(it)
    if bwd:
        dq_ref, dk_ref, dv_ref = next(it), next(it), next(it)
    if turned:
        t_ref = next(it)
    keys, vals, keys_t, vals_t, s_bufs, p_buf, ds_buf = it
    slot = [jnp.bitwise_xor(p, s_ref[1]) for p in range(2)]

    @pl.when(pl.program_id(1) == 0)
    def _():
        for p in range(2):
            kb, vb = k_ref[slot[p]], v_ref[slot[p]]
            keys[rows(p), :] = kb
            vals[rows(p), :] = vb
            keys_t[:, rows(p)] = kb.astype(F32).T.astype(BF16)
            vals_t[:, rows(p)] = vb.astype(F32).T.astype(BF16)
        if bwd:
            dk_ref[...] = jnp.zeros_like(dk_ref)
            dv_ref[...] = jnp.zeros_like(dv_ref)

    iota = functools.partial(lax.broadcasted_iota, jnp.int32, (SUB, SUB))
    causal = iota(0) <= iota(1)
    subs = range(N_SUB)
    tiles = [(i, j) for i in subs for j in range(i + 1)]
    tile = lambda j: slice(SUB * j, SUB * (j + 1))
    per = PIECE // SUB
    base = lambda i, j: tile(i * (i + 1) // 2 + j)
    here = lambda i, h: (slot[i // per], h)
    q = [[q_ref[(*here(i, h), tile(i % per))] for i in subs] for h in range(TRIO)]
    d_o = [[do_ref[(*here(i, h), tile(i % per))] for i in subs] for h in range(TRIO)] if bwd else None

    def phases(h):
        top, inv, total, out_t, delta = {}, {}, {}, {}, {}
        s_buf = s_bufs.at[h]

        def score(i, j):
            s = dot_nt(keys[tile(j), :], q[h][i])
            return jnp.where(causal, s, -jnp.inf) if j == i else s

        def add(sums, i, first, x, f):
            sums[i] = x if first else f(sums[i], x)

        def fold(x, f):
            return f(x.reshape(PART // 8, 8, SUB), axis=0)

        def parts(i, j):
            start = base(i, j).start
            return [(slice(PART * r, PART * (r + 1)), slice(start + PART * r, start + PART * (r + 1))) for r in range(SUB // PART)]

        def scores(i, j):
            s = score(i, j)
            for r, at in parts(i, j):
                s_buf[at, :] = s[r]
                add(top, i, j == 0 and r.start == 0, fold(s[r], jnp.max), jnp.maximum)
            if j == i:
                top[i] = over_keys(jnp.max, top[i])

        def weights(i, j):
            for r, at in parts(i, j):
                p = jnp.exp(s_buf[at, :] - top[i])
                if bwd:
                    s_buf[at, :] = p
                add(total, i, j == 0 and r.start == 0, fold(p, jnp.sum), jnp.add)
                p_buf[h, SUB * j + r.start : SUB * j + r.stop, tile(i)] = p.astype(BF16)
            if j == i:
                width = SUB * (i + 1)
                total[i] = over_keys(jnp.sum, total[i])
                inv[i] = 1.0 / total[i]
                o_t = dot_nn(vals_t[:, :width], p_buf[h, :width, tile(i)]) * inv[i]
                out_t[i] = o_t.astype(BF16)
                o_ref[(*here(i, h), tile(i % per))] = o_t.T.astype(BF16)
                if turned:
                    t_ref[(*here(i, h), 0, ALL, tile(i % per))] = out_t[i]
                if not bwd:
                    ot_ref[(*here(i, h), ALL, tile(i % per))] = out_t[i]
                    lse_ref[h, :, tile(i)] = top[i] + jnp.log(total[i])

        def score_grads(i, j):
            if j == 0:
                o_t = out_t[i] if fwd else ot_ref[(*here(i, h), ALL, tile(i % per))]
                delta[i] = over_keys(jnp.sum, o_t.astype(F32) * d_o[h][i].astype(F32).T)
            s = None if fwd else score(i, j)
            dp = dot_nt(vals[tile(j), :], d_o[h][i])
            for r, at in parts(i, j):
                p = s_buf[at, :] * inv[i] if fwd else jnp.exp(s[r] - lse_ref[h, :, tile(i)])
                to = slice(SUB * j + r.start, SUB * j + r.stop)
                p_buf[h, to, tile(i)] = p.astype(BF16)
                ds_buf[h, to, tile(i)] = (p * (dp[r] - delta[i])).astype(BF16)

        def query_grads(i):
            width = SUB * (i + 1)
            dq = dot_nn(keys_t[:, :width], ds_buf[h, :width, tile(i)]) * SCALE
            low, high, cos, sin = dq[:HALF], dq[HALF:], cos_ref[:, tile(i)], sin_ref[:, tile(i)]
            dq = stack([low * cos + high * sin, high * cos - low * sin])
            dq_ref[(*here(i, h), tile(i % per))] = dq.T.astype(BF16)
            if turned:
                t_ref[(*here(i, h), 1, ALL, tile(i % per))] = dq.astype(BF16)

        def key_grads(j):
            dv_ref[tile(j), :] += dot_nn(p_buf[h, tile(j), SUB * j :], stack(d_o[h][j:]))
            dk_ref[tile(j), :] += dot_nn(ds_buf[h, tile(j), SUB * j :], stack(q[h][j:]))

        each = lambda f, some: [functools.partial(f, *x) for x in some]
        lists = [each(scores, tiles), each(weights, tiles)] if fwd else []
        if bwd:
            alone = [(i,) for i in subs]
            lists += [each(score_grads, tiles), each(query_grads, alone) + each(key_grads, alone)]
        return lists

    work = [phases(h) for h in range(TRIO)]
    n_phases = len(work[0])
    for stage in range(TRIO + n_phases - 1):
        weave(*(work[h][stage - h] for h in range(TRIO) if 0 <= stage - h < n_phases))


def attention(scal, mode, q, k, v, d_o=None, tables=(), saved=(), l0=0, nl=2, turned=None, prior=()):
    n_heads = q.shape[2]
    fwd, bwd = mode != "bwd", mode != "fwd"
    at_in, at_out = lambda l, h, s: (l + l0, 0, h), lambda l, h, s: (l, 0, h)
    block = (None, 2, TRIO, PIECE, E)
    act_in, act = spec(block, at_in), spec(block, at_out)
    flat = spec((None, 2, TRIO, E, PIECE), at_out)
    kv_spec = spec((None, 2, PIECE, E), lambda l, h, s: (l + l0,))
    stat = spec((None, TRIO, 1, ROWS), lambda l, h, s: (l, h))
    acc = spec((None, ROWS, E), lambda l, h, s: (l,))
    ins, specs, outs, out_specs = [q, k, v], [act_in, kv_spec, kv_spec], [], []
    act_shape = struct(BF16, nl, 2, n_heads, PIECE, E)
    if bwd:
        ins += [d_o, *tables]
        specs += [act_in] + [spec((HALF, ROWS))] * 2
    if not fwd:
        ins += saved
        specs += [flat, stat]
    if fwd:
        outs.append(act_shape)
        out_specs.append(act)
    if not bwd:
        outs += [struct(BF16, nl, 2, n_heads, E, PIECE), struct(F32, nl, n_heads, 1, ROWS)]
        out_specs += [flat, stat]
    if bwd:
        outs += [act_shape] + [struct(F32, nl, ROWS, E)] * 2
        out_specs += [act, acc, acc]
    if turned is not None:
        per = GROUP // TRIO
        shift = 0 if turned == OWN else per
        outs.append(struct(BF16, nl, 2, n_heads * (2 if shift else 1), 2, E, PIECE))
        place_head = lambda l, h, s: (l, 0, h + (per * (h // per + turned) if shift else 0))
        out_specs.append(spec((None, 2, TRIO, 2, E, PIECE), place_head))
    aliases = {1 + len(ins): len(outs) - 1} if prior else {}
    ins += prior
    specs += [HBM] * len(prior)
    products = 2 * fwd + 4 * bwd + (not fwd)
    square = TRIO, ROWS, ROWS
    return call(
        functools.partial(attn_body, mode, turned is not None, len(prior)),
        (nl, n_heads // TRIO),
        scal,
        ins,
        specs,
        outs,
        out_specs,
        nl * n_heads * products * 4 * E * SUB * SUB * N_TILE,
        scratch=[pltpu.VMEM((ROWS, E), BF16)] * 2
        + [pltpu.VMEM((E, ROWS), BF16)] * 2
        + [pltpu.VMEM((TRIO, N_TILE * SUB if fwd else SUB, SUB), F32)]
        + [pltpu.VMEM(square, BF16)] * 2,
        aliases=aliases,
    )


def seq_near(s, flip, other):
    return 2 * jnp.bitwise_xor(s[0], flip) + jnp.bitwise_xor(s[1], other)


def combine_body(kind, n_act, n_w, near, fresh, steps, s_ref, *refs):
    acts, ws, refs = refs[:n_act], refs[n_act : n_act + n_w], refs[n_act + n_w :]
    c, n = s_ref[1], pl.program_id(0)
    if kind == "dh":
        kv_refs, refs = refs[:2], refs[2:]
    if not fresh:
        refs = refs[1:]
    finish = []
    if near:
        pieces, theirs, refs = refs[2 : 2 + len(near)], refs[2 + len(near)], refs[len(near) + 3 :]
        *refs, rows_out, grad_out, row_buf, grad_buf, row_sem, grad_sem = refs
        row_chunks = [
            (r.at[cut], rows_out.at[seq_near(s_ref, *at), cut])
            for r, at in zip(pieces, near, strict=True)
            for cut in (pl.ds(SUB * i, SUB) for i in range(PIECE // SUB))
        ]
        grad_chunks = [(theirs.at[i], grad_out.at[GROUP * (1 - c) + i]) for i in range(GROUP)]
        finish.append(in_flight(n, steps, row_chunks, row_buf, row_sem))
        finish.append(in_flight(n, steps, grad_chunks, grad_buf, grad_sem, first=steps - GROUP - 1))
    a = lanes([stack([r[0, h], r[1, h]]) for r in acts for h in range(r.shape[1])])
    held = [ws[0][pl.ds(GROUP * i, GROUP)] for i in (c, 1 - c)] + [w[...] for w in ws[1:]]
    if kind == "out":
        x = dot_nn(a, stack([w.reshape(w.shape[0] * E, w.shape[2]) for w in held]))
    else:
        x = dot_nt(a, lanes([w[h] for w in held for h in range(w.shape[0])] + [r[...] for r in kv_refs]))
    x = x.astype(BF16)
    refs[0][...] = x[rows(0)]
    refs[1][...] = x[rows(1)]
    if fresh:
        refs[2][...] = x[rows(0)]
    for f in finish:
        f()


def combine(scal, kind, l, acts, weights, kv=(), big=None, side=None):
    d = weights[0].shape[2 if kind == "out" else 1]
    steps = d // COLS
    in_specs = [
        spec((None, 2, a.shape[2], PIECE, E), lambda n, s, i=min(l, a.shape[0] - 1): (i,), once=True) for a in acts
    ]
    if kind == "out":
        in_specs += [spec((w.shape[0], E, COLS), lambda n, s: (0, 0, n)) for w in weights]
    else:
        in_specs += [spec((w.shape[0], COLS, E), lambda n, s: (0, n)) for w in weights]
        in_specs += [spec((COLS, E), lambda n, s: (n,))] * 2
    piece = spec((PIECE, COLS), lambda n, s: (0, n))
    fresh = big is None
    ins, aliases, scratch, near = [*acts, *weights, *kv], {}, [], ()
    outs = [struct(BF16, 8, PIECE, d)] + [struct(BF16, PIECE, d)] * (1 + fresh)
    out_specs = [spec((None, PIECE, COLS), lambda n, s: (seq_of(l, s), 0, n))] + [piece] * (1 + fresh)
    moved = [] if fresh else [big]
    if side:
        whole, pieces, near, grad, theirs = side
        moved += [whole, grad, *pieces, theirs]
        outs += [struct(x.dtype, *x.shape) for x in (whole, grad)]
        out_specs += [HBM] * 2
        dma = pltpu.SemaphoreType.DMA
        scratch = [
            pltpu.VMEM((2, SUB, d), BF16),
            pltpu.VMEM((2, *theirs.shape[1:]), F32),
            dma((2, 2)),
            dma((2, 2)),
        ]
    for i, o in zip(range(3 if side else len(moved)), (0, 2, 3), strict=False):
        aliases[1 + len(ins) + i] = o
    return call(
        functools.partial(combine_body, kind, len(acts), len(weights), near, fresh, steps),
        (steps,),
        scal,
        ins + moved,
        in_specs + [HBM] * len(moved),
        outs,
        out_specs,
        2 * ROWS * sum(a.shape[2] for a in acts) * E * d,
        scratch=scratch,
        aliases=aliases,
    )


def dw_local_body(s_ref, t_ref, *refs):
    xs, o_ref = refs[:4], refs[-1]
    a = lanes([stack([t_ref[l, p, h] for h in range(t_ref.shape[2])]) for l in range(2) for p in range(2)])
    o_ref[...] = dot_nn(a, stack([x[...] for x in xs])).reshape(o_ref.shape)


def dw_local(scal, turned, x, x_recv, prior=()):
    d = x.shape[-1]
    steps = d // DW_COLS // 2
    shift = steps * len(prior)
    block = (None, PIECE, DW_COLS)
    rows_at = []
    for l in range(2):
        rows_at.append(spec(block, lambda n, s, l=l: (seq_of(l, s), 0, n + shift)))
        rows_at.append(spec(block, lambda n, s, l=l: (l, 0, n + shift)))
    n_heads = turned.shape[2]
    ins = [turned, x, x_recv, x, x_recv]
    return call(
        dw_local_body,
        (steps,),
        scal,
        [*ins, *prior],
        [spec((2, 2, n_heads, None, E, PIECE)), *rows_at] + [HBM] * len(prior),
        struct(F32, n_heads, E, d),
        spec((n_heads, E, DW_COLS), lambda n, s: (0, 0, n + shift)),
        2 * n_heads * E * ROWS * d,
        aliases={1 + len(ins): 0} if prior else None,
    )


def dw_rest_body(last, s_ref, *refs):
    ts, xs, refs = refs[:8], refs[8:12], refs[12:]
    a = lanes([stack([t[h] for t in ts[2 * g : 2 * g + 2] for h in range(UNIT)]) for g in range(4)])
    acc = dot_nn(a, stack([x[...] for x in xs])).reshape(GROUP, E, DW_COLS) + refs[0][...]
    if last:
        acc = acc + refs[1][...]
    for o in refs[-2:] if last else refs[-1:]:
        o[...] = acc


NEAR = tuple((flip, other) for other in range(2) for flip in (1, 2))


def near_specs(half, which):
    specs = []
    for _, other in NEAR:
        i = half ^ other
        specs += [spec((UNIT, None, E, PIECE), lambda n, s, j=j: (j, which)) for j in (i, 2 + i)]
    rows_at = [spec((None, PIECE, DW_COLS), lambda n, s, at=at: (seq_near(s, *at), 0, n)) for at in NEAR]
    return specs, rows_at


def dw_rest(scal, half, turned, x, local, recv=None):
    d = x.shape[-1]
    block, at_n = (GROUP, E, DW_COLS), lambda n, s: (0, 0, n)
    specs, rows_at = near_specs(half, 0)
    specs += rows_at + [spec(block, lambda n, s: (half, 0, n))]
    ins = [*(t for t in turned for _ in range(2)), x, x, x, x, local]
    outs, out_specs = [struct(F32, GROUP, E, d)], [spec(block, at_n)]
    last = recv is not None
    if last:
        ins.append(recv)
        specs.append(spec(block, at_n))
        outs.insert(0, struct(F32, 2 * GROUP, E, d))
        out_specs.insert(0, spec(block, lambda n, s: (s[1], 0, n)))
    return call(
        functools.partial(dw_rest_body, last),
        (d // DW_COLS,),
        scal,
        ins,
        specs,
        outs,
        out_specs,
        4 * GROUP * E * ROWS * d,
    )


def dw_in_body(last, s_ref, t_ref, u0_ref, u1_ref, *refs):
    ts, kvs, xs, refs = refs[:8], refs[8:12], refs[12:20], refs[20:]
    turn = lambda x: [x.astype(F32).T.astype(BF16)]
    groups = [
        stack([t_ref[l, p, h] for h in range(GROUP)] + turn(u[p]))
        for l, u in enumerate((u0_ref, u1_ref))
        for p in range(2)
    ]
    groups += [
        stack([t[h] for t in ts[2 * g : 2 * g + 2] for h in range(UNIT)] + turn(kv[...])) for g, kv in enumerate(kvs)
    ]
    acc = dot_nn(lanes(groups), stack([x[...] for x in xs])).reshape(GROUP + 1, E, DW_COLS)
    if not last:
        refs[0][...] = acc
        return
    acc = acc + refs[0][...]
    for h in range(GROUP):
        refs[1][h] = refs[2][h] = acc[h].T
    refs[3][...] = acc[GROUP].T


def dw_in(scal, half, turned_0, kv_0, kv_1, turned, kv, x, x_recv, recv=None):
    d = x.shape[-1]
    kv_half = lambda s: jnp.bitwise_xor(half, s[1])
    near, rows_at = near_specs(half, 1)
    local = [spec((2, 2, GROUP, None, E, PIECE), lambda n, s: (0, 0, half, 1))]
    local += [spec((None, 2, None, PIECE, E), lambda n, s: (0, 0, kv_half(s)))] * 2
    block = (None, PIECE, DW_COLS)
    for l in range(2):
        rows_at.insert(2 * l, spec(block, lambda n, s, l=l: (seq_of(l, s), 0, n)))
        rows_at.insert(2 * l + 1, spec(block, lambda n, s, l=l: (l, 0, n)))
    near += [spec((None, PIECE, E), lambda n, s: (kv_half(s),))] * len(kv)
    ins = [turned_0, kv_0, kv_1, *(t for t in turned for _ in range(2)), *kv, x, x_recv, x, x_recv, x, x, x, x]
    specs = local + near + rows_at
    part = spec((GROUP + 1, E, DW_COLS), lambda n, s: (0, 0, n))
    outs, out_specs = [struct(F32, GROUP + 1, E, d)], [part]
    last = recv is not None
    if last:
        ins.append(recv)
        specs.append(part)
        block = (GROUP, DW_COLS, E)
        outs = [struct(F32, 2 * GROUP, d, E), struct(F32, GROUP, d, E), struct(F32, d, E)]
        out_specs = [spec(block, lambda n, s: (s[1], n)), spec(block, lambda n, s: (0, n))]
        out_specs.append(spec((DW_COLS, E), lambda n, s: (n,)))
    return call(
        functools.partial(dw_in_body, last),
        (d // DW_COLS,),
        scal,
        ins,
        specs,
        outs,
        out_specs,
        8 * (GROUP + 1) * E * ROWS * d,
    )


def copy_body(s_ref, x_ref, o_ref):
    o_ref[...] = x_ref[...]


def pick(indices, x, block):
    count, rest = indices.shape[0], x.shape[1:]
    return call(
        copy_body,
        (count,),
        indices,
        [x],
        [spec((block, *rest), lambda i, s: (s[i],))],
        struct(x.dtype, count * block, *rest),
        spec((block, *rest), lambda i, s: (i,)),
        x.size,
    )


def place_body(n, s_ref, *refs):
    for j in range(n):

        @pl.when(pl.program_id(0) == j)
        def _():
            refs[-1][...] = refs[j][...]


def place(seqs, big, pieces):
    n, d = len(pieces), big.shape[-1]
    return call(
        functools.partial(place_body, n),
        (n,),
        seqs,
        [*pieces, big],
        [spec((PIECE, d))] * n + [HBM],
        struct(big.dtype, *big.shape),
        spec((None, PIECE, d), lambda i, s: (s[i],)),
        n * PIECE * d,
        aliases={1 + n: 0},
    )


def after(x, *deps):
    return lax.optimization_barrier((x, *deps))[0]


def solution(mesh):
    n_tp, n_cp = mesh.shape["tp"], mesh.shape["cp"]
    chips = range(n_tp)

    def on_chip(x):
        return lax.ppermute(x, "cp", [(c, n_cp - 1 - c) for c in range(n_cp)])

    def to_chip(x, flip):
        return lax.ppermute(x, "tp", [(i, i ^ flip) for i in chips])

    def to_chip_other(x, flip):
        pairs = [(i * n_cp + c, (i ^ flip) * n_cp + (1 - c)) for i in chips for c in range(n_cp)]
        return lax.ppermute(x, ("tp", "cp"), pairs)

    def to_both(f, x):
        return [f(x, 1), f(x, 2)]

    def spread(m, r):
        return to_both(to_chip, m) + to_both(to_chip_other, r)

    def swap_heads(x):
        return [
            f(x[0, p, 2 * GROUP * i : 2 * GROUP * (i + 1)], 1 + i)
            for p, f in enumerate((to_chip, to_chip_other))
            for i in range(2)
        ]

    def with_partner(ws):
        return [x for w in ws for x in (w, on_chip(w))]

    def relay(w_in, u, dep):
        ws = [after(w_in[a, u], dep) for a in (1, 2)]
        return with_partner(ws), to_chip(ws[u], 2 - u)

    def local_program(hidden, grad, w_query, w_key, w_value, w_out):
        t, c = lax.axis_index("tp"), lax.axis_index("cp")
        chain = [jnp.stack([t, c]).astype(jnp.int32)]

        def step(f, *args, **kw):
            out = f(chain[0], *args, **kw)
            chain[0] = after(chain[0], jax.tree.leaves(out)[0])
            return out

        cos, sin = rope_tables(ROWS)
        tables = [jnp.asarray(np.concatenate(x, axis=1)) for x in ((cos, cos), (-sin, sin))]
        tables_t = [jnp.asarray(np.ascontiguousarray(x.T)) for x in (cos, sin)]
        wq, wo = w_query.transpose(1, 0, 2), w_out
        kv_w = (w_key, w_value)
        own, ext, nx, ny = 2 * t, 2 * (3 - t), 2 * (t ^ 1), 2 * (t ^ 2)
        theirs = jnp.stack([own + 1 - c, ext + 1 - c]).astype(jnp.int32)
        unit = (2 * c).astype(jnp.int32)[None]

        wq_in, wo_in = {}, {}
        sent = pick(theirs, hidden, 1)
        h_recv = on_chip(sent)
        sent = pick(after(unit, sent), wq, UNIT)
        for a in (1, 2):
            wq_in[a, 0] = to_chip(sent, a)
        sent = pick(after(unit, sent), wo, UNIT)
        for a in (1, 2):
            wo_in[a, 0] = to_chip(sent, a)
        g_recv = on_chip(pick(after(theirs, sent), grad, 1))

        q_0, k, v = step(proj, "q", hidden, h_recv, [wq], tables, kv=kv_w)
        do_0, wo_sent, wq_sent = step(proj, "do", grad, g_recv, [wo], side=[wq])
        for a in (1, 2):
            wq_in[a, 1] = to_chip(wq_sent, a)
            wo_in[a, 1] = to_chip(wo_sent, a)
        wq_n0, wq_d0 = relay(wq_in, 0, do_0)
        o_0, dq_0, dk_0, dv_0, t_0 = step(attention, "fused", q_0, k, v, do_0, tables_t, turned=OWN)
        dwo = step(dw_local, t_0, grad, g_recv)

        wo_n0, wo_d0 = relay(wo_in, 0, dwo)
        (q_n0,) = step(proj, "q", hidden, h_recv, wq_n0, tables)
        (do_n0,) = step(proj, "do", grad, g_recv, wo_n0)
        wq_n1, wq_d1 = relay(wq_in, 1, do_n0)
        o_n0, dq_n0, dk_n0, dv_n0, t_n0 = step(attention, "fused", q_n0, k, v, do_n0, tables_t, turned=0)
        (q_n1,) = step(proj, "q", hidden, h_recv, wq_n1, tables)
        wo_n1, wo_d1 = relay(wo_in, 1, q_n1)
        dwo = step(dw_local, t_0, grad, g_recv, prior=[dwo])
        (do_n1,) = step(proj, "do", grad, g_recv, wo_n1)
        wq_d = with_partner([after(w, do_n1) for w in (wq_d0, wq_d1)])
        o_n1, dq_n1, dk_n1, dv_n1, t_n1 = step(attention, "fused", q_n1, k, v, do_n1, tables_t, turned=1, prior=[t_n0])
        t_nb = swap_heads(t_n1)

        (q_d,) = step(proj, "q", hidden, h_recv, wq_d, tables)
        wo_d = with_partner([after(w, q_d) for w in (wo_d0, wo_d1)])
        wo_all = [wo, *wo_n0, *wo_n1, *wo_d]
        wq_all = [wq, *wq_n0, *wq_n1, *wq_d]
        o_d, ot_d, lse_d = step(attention, "fwd", q_d, k, v, nl=1)
        out_big, out_r, out_m = step(combine, "out", 0, [o_0, o_n0, o_n1, o_d], wo_all)
        out_m = to_both(to_chip, out_m)
        (do_d,) = step(proj, "do", grad, g_recv, wo_d)
        dq_d, dk_d, dv_d = step(attention, "bwd", q_d, k, v, do_d, tables_t, saved=[ot_d, lse_d], nl=1)

        def finish_kv(l, *last):
            dk, dv = [
                x[l] + y[l] + z[l] + w[0]
                for x, y, z, w in zip((dk_0, dv_0), (dk_n0, dv_n0), (dk_n1, dv_n1), last, strict=True)
            ]
            dk = dk * tables[0] - jnp.roll(dk, HALF, axis=1) * tables[1]
            x = jnp.stack([dk, dv]).astype(BF16).reshape(2, 2, PIECE, E).transpose(1, 0, 2, 3)
            return jnp.where(c == 0, x, x[::-1])[None]

        dkv_0 = finish_kv(0, dk_d, dv_d)
        kv_nb = spread(dkv_0[0, 0], dkv_0[0, 1])
        out_r = after(out_r, dkv_0)
        out_r = to_both(to_chip_other, out_r) + [on_chip(out_r)]
        dh_big, dh_r, dh_m = step(combine, "dh", 0, [dq_0, dq_n0, dq_n1, dq_d, dkv_0], wq_all, kv=kv_w)
        dh_in = spread(dh_m, dh_r) + [on_chip(dh_r)]

        o_e, dq_e, dk_e, dv_e = step(attention, "fused", q_d, k, v, do_d, tables_t, l0=1, nl=1)
        dkv_1 = finish_kv(1, dk_e, dv_e)

        (wo_part,) = step(dw_rest, 1, t_nb, grad, dwo)
        wo_part = on_chip(wo_part)
        dw_args = t_0, dkv_0, dkv_1, t_nb, kv_nb, hidden, h_recv
        (wq_part,) = step(dw_in, 1, *dw_args)
        wq_part = on_chip(wq_part)
        dwo_big, dwo_mine = step(dw_rest, 0, t_nb, grad, dwo, wo_part)
        dwo_theirs = on_chip(dwo_mine)
        dwq_big, dwq_mine, dkv_mine = step(dw_in, 0, *dw_args, wq_part)
        dwq_theirs = on_chip(dwq_mine)
        dkv_theirs = on_chip(dkv_mine)

        acts = [dq_0, dq_n0, dq_n1, dq_e, dkv_1]
        side = out_big, out_m + out_r, [*NEAR, (0, 1)], dwo_big, dwo_theirs
        dh_big, dh_er, out_big, d_w_out = step(combine, "dh", 1, acts, wq_all, kv=kv_w, big=dh_big, side=side)
        dh_er = on_chip(dh_er)
        early = dh_in[:2] + dh_in[4:]
        side = dh_big, early, [*NEAR[:2], (0, 1)], dwq_big, dwq_theirs
        out_big, out_er, dh_big, dwq = step(combine, "out", 1, [o_0, o_n0, o_n1, o_e], wo_all, big=out_big, side=side)
        out_er = on_chip(out_er)
        late = jnp.stack([nx + 1 - c, ny + 1 - c, ext + 1 - c]).astype(jnp.int32)
        d_hidden = place(after(late, out_big), dh_big, [*dh_in[2:4], dh_er])
        attn_out = place(after(late[2:], d_hidden), out_big, [out_er])
        d_w_key = jnp.where(c == 0, dkv_mine, dkv_theirs)
        d_w_value = jnp.where(c == 0, dkv_theirs, dkv_mine)
        return attn_out, d_hidden, dwq.transpose(1, 0, 2), d_w_key, d_w_value, d_w_out

    row = P(None, "cp", None)
    wq_spec, wo_spec = P(None, "tp", None), P("tp", None, None)
    return jax.shard_map(
        local_program,
        mesh=mesh,
        in_specs=(row, row, wq_spec, P(), P(), wo_spec),
        out_specs=(row, row, wq_spec, P(), P(), wo_spec),
        check_vma=False,
    )
```
